32 devices in a mesh: member: 2 (over y), lat: 4 (over z), lon: 4 (over x, core).
Axes of the slice: x: 2, y: 2, z: 4, core: 2. Of those that a mesh axis runs over, the one named last changes fastest.
Arguments:
- layer_inputs: bfloat16 [2, 256, 192, 512], P('member', None, 'lat', 'lon'), may hold values from -6 to 6
- conv_weight: bfloat16 [3, 3, 69, 256], replicated, may hold values from -0.125 to 0.125
- channel_offset: float32 [69], replicated, may hold values from -4 to 4
- observed: bfloat16 [69, 192, 512], P(None, 'lat', 'lon'), may hold values from -6 to 6
- var_weight: float32 [69], replicated, may hold values from 0.5 to 4
Outputs:
- predicted_fields: bfloat16 [2, 69, 192, 512], P('member', None, 'lat', 'lon')
- input_slope_field: bfloat16 [2, 256, 192, 512], P('member', None, 'lat', 'lon')
The draws below stay inside these ranges and needn't reach their ends.
All inputs are finite; a program needn't handle non-finite values.
Results may differ from the reference program's by a relative error of at most 0.0063.
Values may be sent and summed in bfloat16 or wider, within the bound.
A program may use at most 192 MiB of HBM per device.

```python
import math
import jax
import jax.numpy as jnp
from jax import lax

C = 256
OV = 69
MEMBERS = 2
NLAT = 192
NLON = 512


def steps_of(key, dims, cuts, low, top_value):
    def one(axis_at, shards_of):
        heights = jax.random.uniform(jax.random.fold_in(jax.random.fold_in(key, 6), axis_at), (shards_of,), jnp.float32, low / len(cuts), top_value / len(cuts))
        return jnp.repeat(jnp.exp(heights), dims[axis_at] // shards_of).reshape((-1,) + (1,) * (len(dims) - axis_at - 1))

    loudness = one(*cuts[0])
    for cut in cuts[1:]:
        loudness = loudness * one(*cut)
    return loudness


def gaussian(rng, extent, scale, bound, shards=(), kind=jnp.bfloat16):
    array = jax.random.normal(rng, extent, jnp.float32) * scale
    if len(shards) > 0:
        array = steps_of(rng, extent, shards, -0.22, 0.18) * array
    return jnp.clip(array, min=-bound, max=bound).astype(kind)


def setup_inputs(seed: int = 0) -> dict:
    streams_of = jax.random.split(jax.random.key(seed), 6)
    layer_inputs = gaussian(streams_of[0], (MEMBERS, C, NLAT, NLON), 1.0, 6.0, ((0, 2), (2, 4), (3, 4)))
    conv_weight = gaussian(streams_of[1], (3, 3, OV, C), (9 * C) ** -0.5, 0.125)
    channel_offset = gaussian(streams_of[2], (OV,), 1.0, 4.0, (), jnp.float32)
    observed = gaussian(streams_of[3], (OV, NLAT, NLON), 1.0, 6.0, ((1, 4), (2, 4)))
    var_weight = jnp.clip(jnp.exp(jax.random.uniform(streams_of[4], (OV,), jnp.float32, math.log(0.5), math.log(4.0))), 0.5, 4.0)
    return {"layer_inputs": layer_inputs, "conv_weight": conv_weight, "channel_offset": channel_offset, "observed": observed, "var_weight": var_weight}


smoothing = 0.25

def smooth(difference):
    return difference * lax.rsqrt(difference * difference + smoothing * smoothing)

def cycle_pad(field):
    widened = jnp.concatenate([field[..., -1:], field, field[..., :1]], axis=-1)
    zeros = jnp.zeros_like(widened[..., :1, :])
    return jnp.concatenate([zeros, widened, zeros], axis=-2)

def reference(layer_inputs, conv_weight, channel_offset, observed, var_weight):

    def apply_output_layer(member_features):
        padded = cycle_pad(member_features)
        accumulated_outcome = jnp.zeros((OV, NLAT * NLON), jnp.float32)
        for row_tap in range(3):
            for col_tap in range(3):
                window = padded[:, row_tap:row_tap + NLAT, col_tap:col_tap + NLON].reshape(C, NLAT * NLON)
                accumulated_outcome = accumulated_outcome + jnp.dot(conv_weight[row_tap, col_tap], window, preferred_element_type=jnp.float32)
        return (accumulated_outcome.reshape(OV, NLAT, NLON) + channel_offset[:, None, None]).astype(jnp.bfloat16)
    predicted_fields = lax.map(apply_output_layer, layer_inputs)
    quantity_table = predicted_fields.astype(jnp.float32)

    def add_member(running, member_values):
        return (running + smooth(quantity_table - member_values[None]), None)
    pair_sums, unused = lax.scan(add_member, jnp.zeros_like(quantity_table), quantity_table)
    row_index = jnp.arange(NLAT).astype(jnp.float32)
    lat_weight = jnp.cos((-80.0 + 160.0 * (row_index + 0.5) / NLAT) * (jnp.pi / 180.0))
    target = observed.astype(jnp.float32)[None]
    gradient = (lat_weight[:, None] * var_weight[:, None, None] * (smooth(quantity_table - target) - pair_sums / (MEMBERS - 1))).astype(jnp.bfloat16)

    def backward(member_gradient):
        padded = cycle_pad(member_gradient)
        accumulated_outcome = jnp.zeros((C, NLAT * NLON), jnp.float32)
        for row_tap in range(3):
            for col_tap in range(3):
                window = padded[:, 2 - row_tap:2 - row_tap + NLAT, 2 - col_tap:2 - col_tap + NLON].reshape(OV, NLAT * NLON)
                accumulated_outcome = accumulated_outcome + jnp.dot(conv_weight[row_tap, col_tap].T, window, preferred_element_type=jnp.float32)
        return accumulated_outcome.reshape(C, NLAT, NLON).astype(jnp.bfloat16)
    input_slope_field = lax.map(backward, gradient)
    return (predicted_fields, input_slope_field)
```

```python
import functools

import jax
import jax.numpy as jnp
from jax import lax
from jax.experimental import pallas as pl
from jax.experimental.pallas import tpu as pltpu
from jax.sharding import PartitionSpec as P

MESH = pl.DeviceIdType.MESH
smoothing = 0.25
CHUNK = 16
f32, bf16 = jnp.float32, jnp.bfloat16


def smooth(difference):
    return difference * lax.rsqrt(difference * difference + smoothing * smoothing)


def pitch_of(rows):
    return rows + 1 - rows % 2


def plan(rows):
    pairs, half = rows // 2, CHUNK // 2
    chunks = rows // CHUNK
    if chunks < 3:
        return [list(range(1, pairs - 1)), sorted({0, pairs - 1})]
    base = chunks // 2 * half
    core = list(range(base + 1, base + half - 1))
    cut = lambda run: [run[i : i + 4] for i in range(0, len(run), 4)]
    low = cut(list(range(base, 0, -1)))
    high = cut(list(range(pairs - 2, base + half - 2, -1)))
    groups = [core[:2], core[2:4], low[0], [0, pairs - 1]] + low[1:] + high + [core[4:]]
    return [sorted(g) for g in groups]


def kernel(
    sizes,
    x_hbm, w_hbm, obs_hbm, bias_hbm, var_hbm,
    p_ref, out_ref,
    bias_ref, var_ref,    x_ref, w_ref, obs_ref, load_sem, big, xt, wf, wbt, wb, pf, po, pr, others, ob, gs,
    latw, biasb, varb, edge_out, edge_in, gedge_out, gedge_in,
    row_send, row_recv, grow_send, grow_recv,
    edge_send, edge_recv, gedge_send, gedge_recv, peer_send, peer_recv,
):
    members, lats, lons, channels, rows, cols, outputs, tall, padded = sizes
    pitch = pitch_of(rows)
    chunks = rows // CHUNK
    pairs = rows // 2
    groups = plan(rows)
    place, first = {}, []
    for group in groups:
        first.append(len(place))
        for pair in group:
            place[pair] = len(place)
    last = len(groups) - 1
    middle = chunks // 2
    order = [middle] + [q for q in range(chunks) if q != middle]
    me, lat, lon = lax.axis_index("member"), lax.axis_index("lat"), lax.axis_index("lon")
    right, left = lax.rem(lon + 1, lons), lax.rem(lon + lons - 1, lons)
    has_up, has_down = lat > 0, lat < lats - 1

    loads = {"w": pltpu.make_async_copy(w_hbm, w_ref, load_sem.at[chunks])}
    for q in order:
        loads[q] = pltpu.make_async_copy(
            x_hbm.at[:, pl.ds(q * CHUNK, CHUNK), :], x_ref.at[:, pl.ds(q * CHUNK, CHUNK), :],
            load_sem.at[q])
    loads["bias"] = pltpu.make_async_copy(bias_hbm, bias_ref, load_sem.at[chunks + 2])
    loads["var"] = pltpu.make_async_copy(var_hbm, var_ref, load_sem.at[chunks + 3])
    loads["obs"] = pltpu.make_async_copy(obs_hbm, obs_ref, load_sem.at[chunks + 1])
    for load in loads.values():
        load.start()

    barrier = pltpu.get_barrier_semaphore()
    for side in (left, right):
        pl.semaphore_signal(barrier, inc=1, device_id=(me, lat, side), device_id_type=MESH)

    @pl.when(has_up)
    def _():
        pl.semaphore_signal(barrier, inc=1, device_id=(me, lat - 1, lon), device_id_type=MESH)

    @pl.when(has_down)
    def _():
        pl.semaphore_signal(barrier, inc=1, device_id=(me, lat + 1, lon), device_id_type=MESH)

    def greet(step, carry):
        other = lax.rem(me + step, members)
        pl.semaphore_signal(barrier, inc=1, device_id=(other, lat, lon), device_id_type=MESH)
        return carry

    lax.fori_loop(1, members, greet, 0)

    lane = lax.broadcasted_iota(jnp.int32, (tall, cols), 1)
    at_first, at_last = lane == 0, lane == cols - 1

    biasb[...] = jnp.zeros(biasb.shape, f32)
    varb[...] = jnp.zeros(varb.shape, f32)

    def spread(o, carry):
        biasb[pl.ds(o, 1), :] = jnp.full((1, cols), bias_ref[o], f32)
        varb[pl.ds(o, 1), :] = jnp.full((1, cols), var_ref[o], f32)
        return carry

    wf[...] = jnp.zeros(wf.shape, bf16)

    def blank(r, carry):
        for b in range(3):
            gs[r, b * padded + tall : (b + 1) * padded, :] = jnp.zeros((padded - tall, cols), bf16)
        return carry

    lax.fori_loop(1, rows + 1, blank, 0)
    loads["bias"].wait()
    loads["var"].wait()
    lax.fori_loop(0, outputs, spread, 0, unroll=3)
    loads["w"].wait()
    for a in range(3):
        for b in range(3):
            wf[b * padded : b * padded + outputs, a * channels : (a + 1) * channels] = w_ref[a, b]

    def widen(q):
        loads[q].wait()

        def one(c, carry):
            big[pl.ds(c * pitch + q * CHUNK, CHUNK), :] = (
                x_ref[c, q * CHUNK : (q + 1) * CHUNK, :].astype(f32))
            return carry

        lax.fori_loop(0, channels, one, 0, unroll=16)

    def turn(r, carry):
        xt[r + 1] = big[pl.ds(r, channels, stride=pitch), :].astype(bf16)
        return carry

    def row_copies(array, send, recv):
        up = pltpu.make_async_remote_copy(
            src_ref=array.at[1], dst_ref=array.at[rows + 1], send_sem=send.at[0],
            recv_sem=recv.at[0], device_id=(me, lat - 1, lon), device_id_type=MESH)
        down = pltpu.make_async_remote_copy(
            src_ref=array.at[rows], dst_ref=array.at[0], send_sem=send.at[1],
            recv_sem=recv.at[1], device_id=(me, lat + 1, lon), device_id_type=MESH)
        return up, down

    def start_up(copies):
        pl.when(has_up)(lambda: copies[0].start())

    def start_down(copies):
        pl.when(has_down)(lambda: copies[1].start())

    def wait_rows(copies, array):
        @pl.when(has_up)
        def _():
            copies[1].wait_recv()
            copies[0].wait_send()

        @pl.when(has_down)
        def _():
            copies[0].wait_recv()
            copies[1].wait_send()

        @pl.when(lat == 0)
        def _():
            array[0] = jnp.zeros(array.shape[1:], bf16)

        @pl.when(lat == lats - 1)
        def _():
            array[rows + 1] = jnp.zeros(array.shape[1:], bf16)

    def edge_copies(k, source, target, send, recv):
        return [
            pltpu.make_async_remote_copy(
                src_ref=source.at[k], dst_ref=target.at[k, s], send_sem=send.at[k, s],
                recv_sem=recv.at[k, s], device_id=(me, lat, side), device_id_type=MESH)
            for s, side in enumerate((right, left))]

    def incoming(k, target):
        return jnp.where(lane % 2 == 1, target[k, 0].astype(f32), target[k, 1].astype(f32))

    peer = lambda k, step: pltpu.make_async_remote_copy(
        src_ref=pr.at[pl.ds(first[k], len(groups[k]))],
        dst_ref=others.at[step - 1, pl.ds(first[k], len(groups[k]))],
        send_sem=peer_send.at[k, step - 1], recv_sem=peer_recv.at[k, step - 1],
        device_id=(lax.rem(me + step, members), lat, lon), device_id_type=MESH)

    edges = {}

    def forward(k):
        gather = jnp.zeros((tall, cols), f32)
        for j, pair in enumerate(groups[k]):
            rhs = jnp.concatenate(
                [xt[2 * pair + i : 2 * pair + i + 3].reshape(3 * channels, cols) for i in range(2)],
                axis=1)
            y = jnp.dot(wf[...], rhs, preferred_element_type=f32)
            for i in range(2):
                slot = 2 * j + i
                from_left, mid, from_right = [
                    y[b * padded : b * padded + tall, i * cols : (i + 1) * cols] for b in range(3)]
                from_left = pltpu.roll(from_left, 1, 1)
                from_right = pltpu.roll(from_right, cols - 1, 1)
                both = pltpu.roll(jnp.where(at_first, from_left, from_right), 2 * slot + 1, 1)
                gather = jnp.where(lane // 2 == slot, both, gather)
                total = mid + biasb[...] + jnp.where(at_first, 0.0, from_left)
                pf[2 * pair + i] = total + jnp.where(at_last, 0.0, from_right)
        edge_out[k] = gather.astype(bf16)
        edges[k] = edge_copies(k, edge_out, edge_in, edge_send, edge_recv)
        for copy in edges[k]:
            copy.start()

    def finish(k):
        for copy in edges[k]:
            copy.wait()
        got = incoming(k, edge_in)
        for j, pair in enumerate(groups[k]):
            for i in range(2):
                r, slot = 2 * pair + i, 2 * j + i
                both = pltpu.roll(got, cols - 1 - 2 * slot, 1)
                total = pf[r] + jnp.where(at_first | at_last, both, 0.0)
                po[pl.ds(r, tall, stride=pitch), :] = total
                pr[place[pair], i * tall : (i + 1) * tall, :] = total.astype(bf16)

        def send(step, carry):
            peer(k, step).start()
            return carry

        lax.fori_loop(1, members, send, 0)

    x_rows = row_copies(xt, row_send, row_recv)
    widen(middle)
    lax.fori_loop(middle * CHUNK, (middle + 1) * CHUNK, turn, 0, unroll=2)
    if chunks > 2:
        pl.semaphore_wait(barrier, members + 1 + has_up.astype(jnp.int32) + has_down.astype(jnp.int32))
        forward(0)
    for q in order[1:]:
        widen(q)
        if chunks > 2 and q == 0:
            turn(0, 0)
            start_up(x_rows)
            lax.fori_loop(1, CHUNK, turn, 0, unroll=3)
        elif chunks > 2 and q == chunks - 1:
            turn(rows - 1, 0)
            start_down(x_rows)
            lax.fori_loop(rows - CHUNK, rows - 1, turn, 0, unroll=3)
        else:
            lax.fori_loop(q * CHUNK, (q + 1) * CHUNK, turn, 0, unroll=2)
    if chunks <= 2:
        pl.semaphore_wait(barrier, members + 1 + has_up.astype(jnp.int32) + has_down.astype(jnp.int32))
        start_up(x_rows)
        start_down(x_rows)
        forward(0)
    outer = [k for k, group in enumerate(groups) if 0 in group or pairs - 1 in group]
    inner = [k for k in range(1, last + 1) if k not in outer]
    for n, k in enumerate(inner):
        forward(k)
        if n > 0 and n - 1 < outer[0]:
            finish(n - 1)
    wait_rows(x_rows, xt)
    for k in outer:
        if k > 0:
            forward(k)
    sent = max(len(inner) - 1, 0)

    loads["obs"].wait()

    def unroll_of(n):
        return max(d for d in range(1, 25) if n % d == 0)

    def widen_obs(o, carry):
        ob[pl.ds(o * pitch, rows), :] = obs_ref[o].astype(f32)
        return carry

    lax.fori_loop(0, outputs, widen_obs, 0, unroll=unroll_of(outputs))
    ob[pl.ds(outputs * pitch, (tall - outputs) * pitch), :] = jnp.zeros(
        ((tall - outputs) * pitch, cols), f32)

    wbt[...] = jnp.zeros(wbt.shape, bf16)
    for a in range(3):
        for b in range(3):
            base = ((2 - a) * 3 + b) * padded
            wbt[base : base + outputs, :] = w_ref[a, b]
    wb[...] = jnp.transpose(wbt[...])
    row_index = (lat * rows + lax.broadcasted_iota(jnp.int32, (rows, cols), 0)).astype(f32)
    latw[...] = jnp.cos((-80.0 + 160.0 * (row_index + 0.5) / float(rows * lats)) * (jnp.pi / 180.0))

    for k in range(min(sent, outer[0]), last + 1):
        finish(k)

    def pack(o, carry):
        p_ref[o] = po[pl.ds(o * pitch, rows), :].astype(bf16)
        return carry

    lax.fori_loop(0, outputs, pack, 0, unroll=unroll_of(outputs))
    g_rows = row_copies(gs, grow_send, grow_recv)

    def gradient(k):
        def arrive(step, carry):
            peer(k, step).wait()
            return carry

        lax.fori_loop(1, members, arrive, 0)
        gather = jnp.zeros((tall, cols), f32)
        for j, pair in enumerate(groups[k]):
            at = place[pair]
            for i in range(2):
                r, slot = 2 * pair + i, 2 * j + i
                inside = slice(i * tall, (i + 1) * tall)
                own = pr[at, inside, :].astype(f32)
                misfit = smooth(own - ob[pl.ds(r, tall, stride=pitch), :])
                add = lambda n, run: run + smooth(own - others[n, at, inside, :].astype(f32))
                pair_sum = smooth(own - own)
                if members == 2:
                    pair_sum = add(0, pair_sum)
                else:
                    pair_sum = lax.fori_loop(0, members - 1, add, pair_sum)
                value = latw[r : r + 1, :] * varb[...] * (misfit - pair_sum / (members - 1))
                ahead, behind = pltpu.roll(value, cols - 1, 1), pltpu.roll(value, 1, 1)
                both = pltpu.roll(jnp.where(at_first, behind, ahead), 2 * slot + 1, 1)
                gather = jnp.where(lane // 2 == slot, both, gather)
                gs[r + 1, 0:tall, :] = ahead.astype(bf16)
                gs[r + 1, padded : padded + tall, :] = value.astype(bf16)
                gs[r + 1, 2 * padded : 2 * padded + tall, :] = behind.astype(bf16)
        gedge_out[k] = gather.astype(bf16)
        copies = edge_copies(k, gedge_out, gedge_in, gedge_send, gedge_recv)
        for copy in copies:
            copy.start()
        return copies

    ready, done, packed = set(), set(), set()

    def settle(k, copies):
        for copy in copies:
            copy.wait()
        got = incoming(k, gedge_in)
        for j, pair in enumerate(groups[k]):
            for i in range(2):
                r, slot = 2 * pair + i, 2 * j + i
                both = pltpu.roll(got, cols - 1 - 2 * slot, 1).astype(bf16)
                gs[r + 1, 0:tall, :] = jnp.where(at_last, both, gs[r + 1, 0:tall, :])
                behind = slice(2 * padded, 2 * padded + tall)
                gs[r + 1, behind, :] = jnp.where(at_first, both, gs[r + 1, behind, :])
                ready.add(r)
                if r == 0:
                    start_up(g_rows)
                if r == rows - 1:
                    start_down(g_rows)

    def backward():
        for pair in range(pairs):
            if pair in done or not {2 * pair - 1, 2 * pair, 2 * pair + 1, 2 * pair + 2} <= ready:
                continue
            done.add(pair)
            rhs = jnp.concatenate(
                [gs[2 * pair + i : 2 * pair + i + 3].reshape(9 * padded, cols) for i in range(2)],
                axis=1)
            y = jnp.dot(wb[:, : 9 * padded], rhs, preferred_element_type=f32)
            for i in range(2):
                big[pl.ds(2 * pair + i, channels, stride=pitch), :] = y[:, i * cols : (i + 1) * cols]
        for q in range(chunks):
            if q in packed or not set(range(q * CHUNK // 2, (q + 1) * CHUNK // 2)) <= done:
                continue
            packed.add(q)

            def narrow(c, carry):
                out_ref[c, q * CHUNK : (q + 1) * CHUNK, :] = (
                    big[pl.ds(c * pitch + q * CHUNK, CHUNK), :].astype(bf16))
                return carry

            lax.fori_loop(0, channels, narrow, 0, unroll=16)

    moving = {}
    for k in range(last + 1):
        moving[k] = gradient(k)
        if k > 0 and k - 1 in moving:
            settle(k - 1, moving.pop(k - 1))
            backward()
        if k == last and not set(outer) & {k, k - 1}:
            wait_rows(g_rows, gs)
            ready.update((-1, rows))
            backward()
    settle(last, moving.pop(last))
    if -1 not in ready:
        wait_rows(g_rows, gs)
        ready.update((-1, rows))
    backward()


def shards(layer_inputs, conv_weight, channel_offset, observed, var_weight):
    _, channels, rows, cols = layer_inputs.shape
    outputs = conv_weight.shape[2]
    members, lats, lons = [lax.axis_size(n) for n in ("member", "lat", "lon")]
    tall, padded = -(-outputs // 8) * 8, -(-outputs // 16) * 16
    pairs, count = rows // 2, len(plan(rows))
    chunks, pitch = rows // CHUNK, pitch_of(rows)
    sizes = (members, lats, lons, channels, rows, cols, outputs, tall, padded)
    vmem = pl.BlockSpec(memory_space=pltpu.VMEM)
    hbm = pl.BlockSpec(memory_space=pl.ANY)
    dma = pltpu.SemaphoreType.DMA
    wide = -(-9 * padded // 128) * 128
    predicted, slope = pl.pallas_call(
        functools.partial(kernel, sizes),
        out_shape=(
            pltpu.VMEM((outputs, rows, cols), bf16),
            pltpu.VMEM((channels, rows, cols), bf16),
        ),
        in_specs=[hbm] * 5,
        out_specs=(vmem, vmem),
        scratch_shapes=[
            pltpu.SMEM(channel_offset.shape, f32),
            pltpu.SMEM(var_weight.shape, f32),
            pltpu.VMEM((channels, rows, cols), bf16),
            pltpu.VMEM(conv_weight.shape, bf16),
            pltpu.VMEM((outputs, rows, cols), bf16),
            dma((chunks + 4,)),
            pltpu.VMEM((channels * pitch, cols), f32),
            pltpu.VMEM((rows + 2, channels, cols), bf16),
            pltpu.VMEM((3 * padded, 3 * channels), bf16),
            pltpu.VMEM((wide, channels), bf16),
            pltpu.VMEM((channels, wide), bf16),
            pltpu.VMEM((rows, tall, cols), f32),
            pltpu.VMEM((tall * pitch, cols), f32),
            pltpu.VMEM((pairs, 2 * tall, cols), bf16),
            pltpu.VMEM((members - 1, pairs, 2 * tall, cols), bf16),
            pltpu.VMEM((tall * pitch, cols), f32),
            pltpu.VMEM((rows + 2, 3 * padded, cols), bf16),
            pltpu.VMEM((rows, cols), f32),
            pltpu.VMEM((tall, cols), f32),
            pltpu.VMEM((tall, cols), f32),
            pltpu.VMEM((count, tall, cols), bf16),
            pltpu.VMEM((count, 2, tall, cols), bf16),
            pltpu.VMEM((count, tall, cols), bf16),
            pltpu.VMEM((count, 2, tall, cols), bf16),
            dma((2,)), dma((2,)), dma((2,)), dma((2,)),
            dma((count, 2)), dma((count, 2)), dma((count, 2)), dma((count, 2)),
            dma((count, members - 1)), dma((count, members - 1)),
        ],
        compiler_params=pltpu.CompilerParams(
            collective_id=0, has_side_effects=True, vmem_limit_bytes=60 * 1024 * 1024),
        name="crps_step",
    )(layer_inputs[0], conv_weight, observed, channel_offset, var_weight)
    return predicted[None], slope[None]


def solution(mesh):
    in_specs = (P("member", None, "lat", "lon"), P(), P(), P(None, "lat", "lon"), P())
    out_specs = (P("member", None, "lat", "lon"), P("member", None, "lat", "lon"))
    return jax.shard_map(shards, mesh=mesh, in_specs=in_specs, out_specs=out_specs, check_vma=False)
```

```python
import functools

import jax
import jax.numpy as jnp
from jax import lax
from jax.experimental import pallas as pl
from jax.experimental.pallas import tpu as pltpu
from jax.sharding import PartitionSpec as P

MESH = pl.DeviceIdType.MESH
smoothing = 0.25
CHUNK = 16
f32, bf16 = jnp.float32, jnp.bfloat16


def smooth(difference):
    return difference * lax.rsqrt(difference * difference + smoothing * smoothing)


def pitch_of(rows):
    return rows + 1 - rows % 2


def plan(rows):
    pairs, half = rows // 2, CHUNK // 2
    chunks = rows // CHUNK
    if chunks < 3:
        return [list(range(1, pairs - 1)), sorted({0, pairs - 1})], 1
    base = chunks // 2 * half
    core = list(range(base + 1, base + half - 1))
    low, high = list(range(1, base + 1)), list(range(base + half - 1, pairs - 1))
    cut = lambda run: [run[max(i - 4, 0) : i] for i in range(len(run), 0, -4)]
    early = [core[:2], core[2:4], low[-4:], low[-6:-4]]
    late = [[0, pairs - 1]] + cut(low[:-6]) + cut(high) + [[pair] for pair in core[4:]]
    return [g for g in early if g] + [g for g in late if g], len([g for g in early if g])


def kernel(
    sizes,
    x_hbm, w_hbm, obs_hbm, bias_hbm, var_hbm,
    p_ref, out_ref,
    bias_ref, var_ref, x_ref, w_ref, obs_ref, load_sem, big, xt, wf, wbt, wb, po, pr, others,
    ob, misfits, gs, latw, biasb, varb, partial, border, border_obs, around,
    edge_out, edge_in, rim_out, rim_in, gedge_out, gedge_in,
    row_send, row_recv, grow_send, grow_recv,
    edge_send, edge_recv, rim_send, rim_recv, gedge_send, gedge_recv, peer_send, peer_recv,
):
    members, lats, lons, channels, rows, cols, outputs, tall, padded = sizes
    pitch = pitch_of(rows)
    chunks = rows // CHUNK
    pairs = rows // 2
    groups, ahead_of_rim = plan(rows)
    place, first = {}, []
    for group in groups:
        first.append(len(place))
        for pair in group:
            place[pair] = len(place)
    last = len(groups) - 1
    outer = [k for k, group in enumerate(groups) if 0 in group or pairs - 1 in group]
    inner = [k for k in range(last + 1) if k not in outer]
    middle = chunks // 2
    order = [middle] + [q for q in range(chunks) if q != middle]
    me, lat, lon = lax.axis_index("member"), lax.axis_index("lat"), lax.axis_index("lon")
    right, left = lax.rem(lon + 1, lons), lax.rem(lon + lons - 1, lons)
    has_up, has_down = lat > 0, lat < lats - 1

    barrier = pltpu.get_barrier_semaphore()

    def greet(step, carry):
        other = lax.rem(me + step, members)
        pl.semaphore_signal(barrier, inc=1, device_id=(other, lat, lon), device_id_type=MESH)
        return carry

    lax.fori_loop(1, members, greet, 0)
    for side in (left, right):
        pl.semaphore_signal(barrier, inc=1, device_id=(me, lat, side), device_id_type=MESH)

    @pl.when(has_up)
    def _():
        pl.semaphore_signal(barrier, inc=1, device_id=(me, lat - 1, lon), device_id_type=MESH)

    @pl.when(has_down)
    def _():
        pl.semaphore_signal(barrier, inc=1, device_id=(me, lat + 1, lon), device_id_type=MESH)

    loads = {"w": pltpu.make_async_copy(w_hbm, w_ref, load_sem.at[chunks])}
    for q in order:
        loads[q] = pltpu.make_async_copy(
            x_hbm.at[:, pl.ds(q * CHUNK, CHUNK), :], x_ref.at[:, pl.ds(q * CHUNK, CHUNK), :],
            load_sem.at[q])
    loads["bias"] = pltpu.make_async_copy(bias_hbm, bias_ref, load_sem.at[chunks + 2])
    loads["var"] = pltpu.make_async_copy(var_hbm, var_ref, load_sem.at[chunks + 3])
    loads["obs"] = pltpu.make_async_copy(obs_hbm, obs_ref, load_sem.at[chunks + 1])
    for load in loads.values():
        load.start()

    lane = lax.broadcasted_iota(jnp.int32, (tall, cols), 1)
    at_first, at_last = lane == 0, lane == cols - 1
    at_ends = at_first | at_last
    odd = lane % 2 == 1

    biasb[...] = jnp.zeros(biasb.shape, f32)
    varb[...] = jnp.zeros(varb.shape, f32)

    def spread(o, carry):
        biasb[pl.ds(o, 1), :] = jnp.full((1, cols), bias_ref[o], f32)
        varb[pl.ds(o, 1), :] = jnp.full((1, cols), var_ref[o], f32)
        return carry

    wf[...] = jnp.zeros(wf.shape, bf16)
    for array in (border, border_obs):
        array[...] = jnp.zeros(array.shape, f32)

    def blank(r, carry):
        for b in range(3):
            gs[r, b * padded + tall : (b + 1) * padded, :] = jnp.zeros((padded - tall, cols), bf16)
        return carry

    lax.fori_loop(1, rows + 1, blank, 0)
    loads["bias"].wait()
    loads["var"].wait()
    lax.fori_loop(0, outputs, spread, 0, unroll=3)
    loads["w"].wait()
    for a in range(3):
        for b in range(3):
            wf[b * padded : b * padded + outputs, a * channels : (a + 1) * channels] = w_ref[a, b]

    def unroll_of(n):
        return max(d for d in range(1, 25) if n % d == 0)

    def widen(q):
        loads[q].wait()

        def one(c, carry):
            big[pl.ds(c * pitch + q * CHUNK, CHUNK), :] = (
                x_ref[c, q * CHUNK : (q + 1) * CHUNK, :].astype(f32))
            return carry

        lax.fori_loop(0, channels, one, 0, unroll=16)

    def turn(r, carry):
        xt[r + 1] = big[pl.ds(r, channels, stride=pitch), :].astype(bf16)
        return carry

    def row_copies(array, send, recv):
        up = pltpu.make_async_remote_copy(
            src_ref=array.at[1], dst_ref=array.at[rows + 1], send_sem=send.at[0],
            recv_sem=recv.at[0], device_id=(me, lat - 1, lon), device_id_type=MESH)
        down = pltpu.make_async_remote_copy(
            src_ref=array.at[rows], dst_ref=array.at[0], send_sem=send.at[1],
            recv_sem=recv.at[1], device_id=(me, lat + 1, lon), device_id_type=MESH)
        return up, down

    def start_up(copies):
        pl.when(has_up)(lambda: copies[0].start())

    def start_down(copies):
        pl.when(has_down)(lambda: copies[1].start())

    def wait_rows(copies, array):
        @pl.when(has_up)
        def _():
            copies[1].wait_recv()
            copies[0].wait_send()

        @pl.when(has_down)
        def _():
            copies[0].wait_recv()
            copies[1].wait_send()

        @pl.when(lat == 0)
        def _():
            array[0] = jnp.zeros(array.shape[1:], bf16)

        @pl.when(lat == lats - 1)
        def _():
            array[rows + 1] = jnp.zeros(array.shape[1:], bf16)

    def edge_copies(source, target, send, recv):
        return [
            pltpu.make_async_remote_copy(
                src_ref=source, dst_ref=target.at[s], send_sem=send.at[s],
                recv_sem=recv.at[s], device_id=(me, lat, side), device_id_type=MESH)
            for s, side in enumerate((right, left))]

    def to_peers(act):
        def one(step, carry):
            act(step)
            return carry

        lax.fori_loop(1, members, one, 0)

    peer = lambda k, step: pltpu.make_async_remote_copy(
        src_ref=pr.at[pl.ds(first[k], len(groups[k]))],
        dst_ref=others.at[step - 1, pl.ds(first[k], len(groups[k]))],
        send_sem=peer_send.at[k, step - 1], recv_sem=peer_recv.at[k, step - 1],
        device_id=(lax.rem(me + step, members), lat, lon), device_id_type=MESH)
    rim = lambda step: pltpu.make_async_remote_copy(
        src_ref=rim_out, dst_ref=rim_in.at[step - 1],
        send_sem=rim_send.at[step - 1], recv_sem=rim_recv.at[step - 1],
        device_id=(lax.rem(me + step, members), lat, lon), device_id_type=MESH)
    edges = [
        edge_copies(edge_out.at[n], edge_in.at[n], edge_send.at[n], edge_recv.at[n])
        for n in range(2)]
    gedges = edge_copies(gedge_out, gedge_in, gedge_send, gedge_recv)

    def rows_of(k):
        return [(pair, i, 2 * pair + i) for pair in groups[k] for i in range(2)]

    def forward(k):
        share = jnp.zeros((tall, cols), f32)
        own = jnp.zeros((tall, cols), f32)
        for pair in groups[k]:
            rhs = jnp.concatenate(
                [xt[2 * pair + i : 2 * pair + i + 3].reshape(3 * channels, cols) for i in range(2)],
                axis=1)
            y = jnp.dot(wf[...], rhs, preferred_element_type=f32)
            for i in range(2):
                r = 2 * pair + i
                from_left, mid, from_right = [
                    y[b * padded : b * padded + tall, i * cols : (i + 1) * cols] for b in range(3)]
                from_left = pltpu.roll(from_left, 1, 1)
                from_right = pltpu.roll(from_right, cols - 1, 1)
                total = mid + biasb[...] + jnp.where(at_first, 0.0, from_left)
                total = total + jnp.where(at_last, 0.0, from_right)
                pr[place[pair], i * tall : (i + 1) * tall, :] = total.astype(bf16)
                both = pltpu.roll(jnp.where(at_first, from_left, from_right), 2 * r + 1, 1)
                mine = lane // 2 == r
                share = jnp.where(mine, both, share)
                own = jnp.where(mine, pltpu.roll(total, 2 * r + 1, 1), own)
        at = 1 if k in outer else 0
        partial[at] = share if k in (outer[0], inner[0]) else partial[at] + share
        border[...] = border[...] + own

    def exchange(n):
        edge_out[n] = partial[n].astype(bf16)
        for copy in edges[n]:
            copy.start()

    def enter():
        pl.semaphore_wait(barrier, members + 1 + has_up.astype(jnp.int32) + has_down.astype(jnp.int32))

    x_rows = row_copies(xt, row_send, row_recv)
    fast = inner[:2] if chunks > 2 else []
    widen(middle)
    lax.fori_loop(middle * CHUNK, (middle + 1) * CHUNK, turn, 0, unroll=2)
    for k in fast:
        forward(k)
    for q in order[1:]:
        widen(q)
        lax.fori_loop(q * CHUNK, (q + 1) * CHUNK, turn, 0, unroll=2)
    enter()
    for k in fast:
        to_peers(lambda step: peer(k, step).start())
    start_up(x_rows)
    start_down(x_rows)
    for k in inner:
        if k not in fast:
            forward(k)
            if k < ahead_of_rim:
                to_peers(lambda step: peer(k, step).start())
    exchange(0)

    loads["obs"].wait()

    def widen_obs(o, carry):
        ob[pl.ds(o * pitch, rows), :] = obs_ref[o].astype(f32)
        return carry

    lax.fori_loop(0, outputs, widen_obs, 0, unroll=unroll_of(outputs))
    ob[pl.ds(outputs * pitch, (tall - outputs) * pitch), :] = jnp.zeros(
        ((tall - outputs) * pitch, cols), f32)
    wait_rows(x_rows, xt)
    for k in outer:
        forward(k)
    exchange(1)

    wbt[...] = jnp.zeros(wbt.shape, bf16)
    for a in range(3):
        for b in range(3):
            base = ((2 - a) * 3 + b) * padded
            wbt[base : base + outputs, :] = w_ref[a, b]
    wb[...] = jnp.transpose(wbt[...])

    def latitude(row):
        row_index = (lat * rows + row).astype(f32)
        return jnp.cos((-80.0 + 160.0 * (row_index + 0.5) / float(rows * lats)) * (jnp.pi / 180.0))

    latw[0:rows, :] = latitude(lax.broadcasted_iota(jnp.int32, (rows, cols), 0))
    latw[rows : rows + 8, :] = latitude(lax.broadcasted_iota(jnp.int32, (8, cols), 1) // 2)

    def gather_obs(k):
        own = jnp.zeros((tall, cols), f32)
        for _, _, r in rows_of(k):
            turned = pltpu.roll(ob[pl.ds(r, tall, stride=pitch), :], 2 * r + 1, 1)
            own = jnp.where(lane // 2 == r, turned, own)
        border_obs[...] = border_obs[...] + own

    for k in range(last + 1):
        gather_obs(k)

    arrived = jnp.zeros((tall, cols), f32)
    for n in range(2):
        for copy in edges[n]:
            copy.wait()
        arrived = arrived + jnp.where(odd, edge_in[n, 0].astype(f32), edge_in[n, 1].astype(f32))
    rim_out[...] = (border[...] + arrived).astype(bf16)
    to_peers(lambda step: rim(step).start())
    for k in range(last + 1):
        if k >= ahead_of_rim or k in outer:
            to_peers(lambda step: peer(k, step).start())

    def complete(k):
        rim_own = rim_out[...].astype(f32)
        for pair, i, r in rows_of(k):
            own = pr[place[pair], i * tall : (i + 1) * tall, :].astype(f32)
            own = jnp.where(at_ends, pltpu.roll(rim_own, cols - 1 - 2 * r, 1), own)
            misfits[r] = smooth(own - ob[pl.ds(r, tall, stride=pitch), :])
            po[pl.ds(r, tall, stride=pitch), :] = own

    for k in range(last + 1):
        complete(k)

    def pack(o, carry):
        p_ref[o] = po[pl.ds(o * pitch, rows), :].astype(bf16)
        return carry

    lax.fori_loop(0, outputs, pack, 0, unroll=unroll_of(outputs))

    def spread_sum(own, other):
        add = lambda n, run: run + smooth(own - other(n))
        pair_sum = smooth(own - own)
        if members == 2:
            pair_sum = add(0, pair_sum)
        else:
            pair_sum = lax.fori_loop(0, members - 1, add, pair_sum)
        return pair_sum / (members - 1)

    to_peers(lambda step: rim(step).wait())
    rim_own = rim_out[...].astype(f32)
    value = smooth(rim_own - border_obs[...]) - spread_sum(rim_own, lambda n: rim_in[n].astype(f32))
    value = latw[rows : rows + 1, :] * varb[...] * value
    value = jnp.where(odd, pltpu.roll(value, 1, 1), pltpu.roll(value, cols - 1, 1))
    gedge_out[...] = value.astype(bf16)
    for copy in gedges:
        copy.start()
    for copy in gedges:
        copy.wait()
    around[...] = jnp.where(odd, gedge_in[0].astype(f32), gedge_in[1].astype(f32))

    g_rows = row_copies(gs, grow_send, grow_recv)
    ready, done, packed = set(), set(), set()

    def gradient(k):
        to_peers(lambda step: peer(k, step).wait())
        for pair, i, r in rows_of(k):
            at, inside = place[pair], slice(i * tall, (i + 1) * tall)

            def other(n):
                patch = pltpu.roll(rim_in[n].astype(f32), cols - 1 - 2 * r, 1)
                return jnp.where(at_ends, patch, others[n, at, inside, :].astype(f32))

            own = po[pl.ds(r, tall, stride=pitch), :].astype(bf16).astype(f32)
            value = latw[r : r + 1, :] * varb[...] * (misfits[r] - spread_sum(own, other))
            both = pltpu.roll(around[...], cols - 1 - 2 * r, 1)
            ahead = jnp.where(at_last, both, pltpu.roll(value, cols - 1, 1))
            behind = jnp.where(at_first, both, pltpu.roll(value, 1, 1))
            gs[r + 1, 0:tall, :] = ahead.astype(bf16)
            gs[r + 1, padded : padded + tall, :] = value.astype(bf16)
            gs[r + 1, 2 * padded : 2 * padded + tall, :] = behind.astype(bf16)
            ready.add(r)
        if 0 in groups[k]:
            start_up(g_rows)
        if pairs - 1 in groups[k]:
            start_down(g_rows)

    def backward():
        for pair in range(pairs):
            if pair in done or not {2 * pair - 1, 2 * pair, 2 * pair + 1, 2 * pair + 2} <= ready:
                continue
            done.add(pair)
            rhs = jnp.concatenate(
                [gs[2 * pair + i : 2 * pair + i + 3].reshape(9 * padded, cols) for i in range(2)],
                axis=1)
            y = jnp.dot(wb[:, : 9 * padded], rhs, preferred_element_type=f32)
            for i in range(2):
                big[pl.ds(2 * pair + i, channels, stride=pitch), :] = y[:, i * cols : (i + 1) * cols]
        for q in range(chunks):
            if q in packed or not set(range(q * CHUNK // 2, (q + 1) * CHUNK // 2)) <= done:
                continue
            packed.add(q)

            def narrow(c, carry):
                out_ref[c, q * CHUNK : (q + 1) * CHUNK, :] = (
                    big[pl.ds(c * pitch + q * CHUNK, CHUNK), :].astype(bf16))
                return carry

            lax.fori_loop(0, channels, narrow, 0, unroll=16)

    for k in range(last + 1):
        if k == last - 1 and -1 not in ready and outer[-1] < k:
            wait_rows(g_rows, gs)
            ready.update((-1, rows))
            backward()
        gradient(k)
        backward()
    if -1 not in ready:
        wait_rows(g_rows, gs)
        ready.update((-1, rows))
        backward()


def shards(layer_inputs, conv_weight, channel_offset, observed, var_weight):
    _, channels, rows, cols = layer_inputs.shape
    outputs = conv_weight.shape[2]
    members, lats, lons = [lax.axis_size(n) for n in ("member", "lat", "lon")]
    tall, padded = -(-outputs // 8) * 8, -(-outputs // 16) * 16
    pairs, count = rows // 2, len(plan(rows)[0])
    flat = pltpu.VMEM((tall, cols), f32)
    chunks, pitch = rows // CHUNK, pitch_of(rows)
    sizes = (members, lats, lons, channels, rows, cols, outputs, tall, padded)
    vmem = pl.BlockSpec(memory_space=pltpu.VMEM)
    hbm = pl.BlockSpec(memory_space=pl.ANY)
    dma = pltpu.SemaphoreType.DMA
    wide = -(-9 * padded // 128) * 128
    predicted, slope = pl.pallas_call(
        functools.partial(kernel, sizes),
        out_shape=(
            pltpu.VMEM((outputs, rows, cols), bf16),
            pltpu.VMEM((channels, rows, cols), bf16),
        ),
        in_specs=[hbm] * 5,
        out_specs=(vmem, vmem),
        scratch_shapes=[
            pltpu.SMEM(channel_offset.shape, f32),
            pltpu.SMEM(var_weight.shape, f32),
            pltpu.VMEM((channels, rows, cols), bf16),
            pltpu.VMEM(conv_weight.shape, bf16),
            pltpu.VMEM((outputs, rows, cols), bf16),
            dma((chunks + 4,)),
            pltpu.VMEM((channels * pitch, cols), f32),
            pltpu.VMEM((rows + 2, channels, cols), bf16),
            pltpu.VMEM((3 * padded, 3 * channels), bf16),
            pltpu.VMEM((wide, channels), bf16),
            pltpu.VMEM((channels, wide), bf16),
            pltpu.VMEM((tall * pitch, cols), f32),
            pltpu.VMEM((pairs, 2 * tall, cols), bf16),
            pltpu.VMEM((members - 1, pairs, 2 * tall, cols), bf16),
            pltpu.VMEM((tall * pitch, cols), f32),
            pltpu.VMEM((rows, tall, cols), f32),
            pltpu.VMEM((rows + 2, 3 * padded, cols), bf16),
            pltpu.VMEM((rows + 8, cols), f32),
            flat, flat, pltpu.VMEM((2, tall, cols), f32), flat, flat, flat,
            pltpu.VMEM((2, tall, cols), bf16),
            pltpu.VMEM((2, 2, tall, cols), bf16),
            pltpu.VMEM((tall, cols), bf16),
            pltpu.VMEM((members - 1, tall, cols), bf16),
            pltpu.VMEM((tall, cols), bf16),
            pltpu.VMEM((2, tall, cols), bf16),
            dma((2,)), dma((2,)), dma((2,)), dma((2,)),
            dma((2, 2)), dma((2, 2)), dma((members - 1,)), dma((members - 1,)), dma((2,)), dma((2,)),
            dma((count, members - 1)), dma((count, members - 1)),
        ],
        compiler_params=pltpu.CompilerParams(
            collective_id=0, has_side_effects=True, vmem_limit_bytes=60 * 1024 * 1024),
        name="crps_step",
    )(layer_inputs[0], conv_weight, observed, channel_offset, var_weight)
    return predicted[None], slope[None]


def solution(mesh):
    in_specs = (P("member", None, "lat", "lon"), P(), P(), P(None, "lat", "lon"), P())
    out_specs = (P("member", None, "lat", "lon"), P("member", None, "lat", "lon"))
    return jax.shard_map(shards, mesh=mesh, in_specs=in_specs, out_specs=out_specs, check_vma=False)
```

```python
import functools

import jax
import jax.numpy as jnp
from jax import lax
from jax.experimental import pallas as pl
from jax.experimental.pallas import tpu as pltpu
from jax.sharding import PartitionSpec as P

MESH = pl.DeviceIdType.MESH
smoothing = 0.25
CHUNK = 16
TILE = 8
ROOM = 67_043_328
f32, bf16 = jnp.float32, jnp.bfloat16


def smooth(difference):
    return difference * lax.rsqrt(difference * difference + smoothing * smoothing)


def pitch_of(rows):
    return rows + 1 - rows % 2


def plan(rows):
    pairs, half = rows // 2, CHUNK // 2
    chunks = rows // CHUNK
    if chunks < 3:
        return [list(range(1, pairs - 1)), sorted({0, pairs - 1})], 1
    base = chunks // 2 * half
    core = list(range(base + 1, base + half - 1))
    low, high = list(range(1, base + 1)), list(range(base + half - 1, pairs - 1))
    cut = lambda run: [run[max(i - 4, 0) : i] for i in range(len(run), 0, -4)]
    early = [core[:1], core[1:2], core[2:4], low[-4:], low[-8:-4]]
    late = [[0, pairs - 1]] + cut(low[:-8]) + cut(high) + [[pair] for pair in core[4:]]
    return [g for g in early if g] + [g for g in late if g], len([g for g in early if g])


def kernel(
    sizes,
    x_hbm, w_hbm, obs_hbm, bias_hbm, var_hbm,
    p_ref, out_ref, big,
    bias_ref, var_ref, x_ref, w_ref, obs_ref, load_sem, xt, wf, wbt, wb, po, pr, others,
    ob, misfits, gs, latw, biasb, varb, partial, border, border_obs, around,
    edge_out, edge_in, rim_out, rim_in, gedge_out, gedge_in,
    row_send, row_recv, grow_send, grow_recv,
    edge_send, edge_recv, rim_send, rim_recv, gedge_send, gedge_recv, peer_send, peer_recv,
):
    members, lats, lons, channels, rows, cols, outputs, tall, padded = sizes
    pitch = pitch_of(rows)
    chunks = rows // CHUNK
    pairs = rows // 2
    groups, ahead_of_rim = plan(rows)
    place, first = {}, []
    for group in groups:
        first.append(len(place))
        for pair in group:
            place[pair] = len(place)
    last = len(groups) - 1
    outer = [k for k, group in enumerate(groups) if 0 in group or pairs - 1 in group]
    inner = [k for k in range(last + 1) if k not in outer]
    tiles = rows // TILE
    start = groups[0][0] * 2 // TILE if chunks > 2 else 0
    order = [start, 0, tiles - 1] + [t + start for t in range(1, tiles - start)]
    order = list(dict.fromkeys(order + list(range(start, -1, -1))))
    me, lat, lon = lax.axis_index("member"), lax.axis_index("lat"), lax.axis_index("lon")
    right, left = lax.rem(lon + 1, lons), lax.rem(lon + lons - 1, lons)
    has_up, has_down = lat > 0, lat < lats - 1

    barrier = pltpu.get_barrier_semaphore()

    def greet(step, carry):
        other = lax.rem(me + step, members)
        pl.semaphore_signal(barrier, inc=1, device_id=(other, lat, lon), device_id_type=MESH)
        return carry

    lax.fori_loop(1, members, greet, 0)
    for side in (left, right):
        pl.semaphore_signal(barrier, inc=1, device_id=(me, lat, side), device_id_type=MESH)

    @pl.when(has_up)
    def _():
        pl.semaphore_signal(barrier, inc=1, device_id=(me, lat - 1, lon), device_id_type=MESH)

    @pl.when(has_down)
    def _():
        pl.semaphore_signal(barrier, inc=1, device_id=(me, lat + 1, lon), device_id_type=MESH)

    loads = {"w": pltpu.make_async_copy(w_hbm, w_ref, load_sem.at[tiles])}
    for q in order:
        loads[q] = pltpu.make_async_copy(
            x_hbm.at[:, pl.ds(q * TILE, TILE), :], x_ref.at[:, pl.ds(q * TILE, TILE), :],
            load_sem.at[q])
    loads["bias"] = pltpu.make_async_copy(bias_hbm, bias_ref, load_sem.at[tiles + 2])
    loads["var"] = pltpu.make_async_copy(var_hbm, var_ref, load_sem.at[tiles + 3])
    loads["obs"] = pltpu.make_async_copy(obs_hbm, obs_ref, load_sem.at[tiles + 1])
    for load in loads.values():
        load.start()

    lane = lax.broadcasted_iota(jnp.int32, (tall, cols), 1)
    at_first, at_last = lane == 0, lane == cols - 1
    at_ends = at_first | at_last
    odd = lane % 2 == 1

    def spread(array, source):
        array[...] = jnp.zeros(array.shape, f32)

        def one(o, carry):
            array[pl.ds(o, 1), :] = jnp.full((1, cols), source[o], f32)
            return carry

        lax.fori_loop(0, outputs, one, 0, unroll=3)

    wf[...] = jnp.zeros(wf.shape, bf16)
    border[...] = jnp.zeros(border.shape, f32)
    loads["bias"].wait()
    spread(biasb, bias_ref)

    def unroll_of(n):
        return max(d for d in range(1, 25) if n % d == 0)

    def turn(r, carry):
        xt[r + 1] = big[pl.ds(r, channels, stride=pitch), :].astype(bf16)
        return carry

    def bring(t):
        loads[t].wait()

        def one(c, carry):
            big[pl.ds(c * pitch + t * TILE, TILE), :] = (
                x_ref[c, t * TILE : (t + 1) * TILE, :].astype(f32))
            return carry

        lax.fori_loop(0, channels, one, 0, unroll=16)
        lax.fori_loop(t * TILE, (t + 1) * TILE, turn, 0, unroll=4)

    def row_copies(array, send, recv):
        up = pltpu.make_async_remote_copy(
            src_ref=array.at[1], dst_ref=array.at[rows + 1], send_sem=send.at[0],
            recv_sem=recv.at[0], device_id=(me, lat - 1, lon), device_id_type=MESH)
        down = pltpu.make_async_remote_copy(
            src_ref=array.at[rows], dst_ref=array.at[0], send_sem=send.at[1],
            recv_sem=recv.at[1], device_id=(me, lat + 1, lon), device_id_type=MESH)
        return up, down

    def start_up(copies):
        pl.when(has_up)(lambda: copies[0].start())

    def start_down(copies):
        pl.when(has_down)(lambda: copies[1].start())

    def wait_rows(copies, array):
        @pl.when(has_up)
        def _():
            copies[1].wait_recv()
            copies[0].wait_send()

        @pl.when(has_down)
        def _():
            copies[0].wait_recv()
            copies[1].wait_send()

        @pl.when(lat == 0)
        def _():
            array[0] = jnp.zeros(array.shape[1:], bf16)

        @pl.when(lat == lats - 1)
        def _():
            array[rows + 1] = jnp.zeros(array.shape[1:], bf16)

    def edge_copies(source, target, send, recv):
        return [
            pltpu.make_async_remote_copy(
                src_ref=source, dst_ref=target.at[s], send_sem=send.at[s],
                recv_sem=recv.at[s], device_id=(me, lat, side), device_id_type=MESH)
            for s, side in enumerate((right, left))]

    def to_peers(act):
        def one(step, carry):
            act(step)
            return carry

        lax.fori_loop(1, members, one, 0)

    peer = lambda k, step: pltpu.make_async_remote_copy(
        src_ref=pr.at[pl.ds(first[k], len(groups[k]))],
        dst_ref=others.at[step - 1, pl.ds(first[k], len(groups[k]))],
        send_sem=peer_send.at[k, step - 1], recv_sem=peer_recv.at[k, step - 1],
        device_id=(lax.rem(me + step, members), lat, lon), device_id_type=MESH)
    rim = lambda step: pltpu.make_async_remote_copy(
        src_ref=rim_out, dst_ref=rim_in.at[step - 1],
        send_sem=rim_send.at[step - 1], recv_sem=rim_recv.at[step - 1],
        device_id=(lax.rem(me + step, members), lat, lon), device_id_type=MESH)
    edges = [
        edge_copies(edge_out.at[n], edge_in.at[n], edge_send.at[n], edge_recv.at[n])
        for n in range(2)]
    gedges = edge_copies(gedge_out, gedge_in, gedge_send, gedge_recv)

    def rows_of(k):
        return [(pair, i, 2 * pair + i) for pair in groups[k] for i in range(2)]

    def forward(k):
        share = jnp.zeros((tall, cols), f32)
        own = jnp.zeros((tall, cols), f32)
        for pair in groups[k]:
            rhs = jnp.concatenate(
                [xt[2 * pair + i : 2 * pair + i + 3].reshape(3 * channels, cols) for i in range(2)],
                axis=1)
            y = jnp.dot(wf[...], rhs, preferred_element_type=f32)
            for i in range(2):
                r = 2 * pair + i
                from_left, mid, from_right = [
                    y[b * padded : b * padded + tall, i * cols : (i + 1) * cols] for b in range(3)]
                from_left = pltpu.roll(from_left, 1, 1)
                from_right = pltpu.roll(from_right, cols - 1, 1)
                total = mid + biasb[...] + jnp.where(at_first, 0.0, from_left)
                total = total + jnp.where(at_last, 0.0, from_right)
                pr[place[pair], i * tall : (i + 1) * tall, :] = total.astype(bf16)
                both = pltpu.roll(jnp.where(at_first, from_left, from_right), 2 * r + 1, 1)
                mine = lane // 2 == r
                share = jnp.where(mine, both, share)
                own = jnp.where(mine, pltpu.roll(total, 2 * r + 1, 1), own)
        at = 1 if k in outer else 0
        partial[at] = share if k in (outer[0], inner[0]) else partial[at] + share
        border[...] = border[...] + own

    def exchange(n):
        edge_out[n] = partial[n].astype(bf16)
        for copy in edges[n]:
            copy.start()

    def enter():
        pl.semaphore_wait(barrier, members + 1 + has_up.astype(jnp.int32) + has_down.astype(jnp.int32))

    x_rows = row_copies(xt, row_send, row_recv)
    waiting = list(order)
    bring(waiting.pop(0))
    loads["w"].wait()
    for a in range(3):
        for b in range(3):
            wf[b * padded : b * padded + outputs, a * channels : (a + 1) * channels] = w_ref[a, b]
    for n, k in enumerate(inner):
        needed = {r // TILE for pair in groups[k] for r in range(2 * pair - 1, 2 * pair + 3)}
        while needed & set(waiting):
            bring(waiting.pop(0))
        forward(k)
        if n == 0:
            enter()
        if k < ahead_of_rim:
            to_peers(lambda step: peer(k, step).start())
        if n == min(1, len(inner) - 1):
            while {0, tiles - 1} & set(waiting):
                bring(waiting.pop(0))
            start_up(x_rows)
            start_down(x_rows)
    exchange(0)

    border_obs[...] = jnp.zeros(border_obs.shape, f32)
    loads["var"].wait()
    spread(varb, var_ref)

    def blank(r, carry):
        for b in range(3):
            gs[r, b * padded + tall : (b + 1) * padded, :] = jnp.zeros((padded - tall, cols), bf16)
        return carry

    lax.fori_loop(1, rows + 1, blank, 0)
    loads["obs"].wait()

    def widen_obs(o, carry):
        ob[pl.ds(o * pitch, rows), :] = obs_ref[o].astype(f32)
        return carry

    lax.fori_loop(0, outputs, widen_obs, 0, unroll=unroll_of(outputs))
    ob[pl.ds(outputs * pitch, (tall - outputs) * pitch), :] = jnp.zeros(
        ((tall - outputs) * pitch, cols), f32)
    wait_rows(x_rows, xt)
    for k in outer:
        forward(k)
    exchange(1)

    wbt[...] = jnp.zeros(wbt.shape, bf16)
    for a in range(3):
        for b in range(3):
            base = ((2 - a) * 3 + b) * padded
            wbt[base : base + outputs, :] = w_ref[a, b]
    wb[...] = jnp.transpose(wbt[...])

    def latitude(row):
        row_index = (lat * rows + row).astype(f32)
        return jnp.cos((-80.0 + 160.0 * (row_index + 0.5) / float(rows * lats)) * (jnp.pi / 180.0))

    latw[0:rows, :] = latitude(lax.broadcasted_iota(jnp.int32, (rows, cols), 0))
    latw[rows : rows + 8, :] = latitude(lax.broadcasted_iota(jnp.int32, (8, cols), 1) // 2)

    def gather_obs(k):
        own = jnp.zeros((tall, cols), f32)
        for _, _, r in rows_of(k):
            turned = pltpu.roll(ob[pl.ds(r, tall, stride=pitch), :], 2 * r + 1, 1)
            own = jnp.where(lane // 2 == r, turned, own)
        border_obs[...] = border_obs[...] + own

    for k in range(last + 1):
        gather_obs(k)

    arrived = jnp.zeros((tall, cols), f32)
    for n in range(2):
        for copy in edges[n]:
            copy.wait()
        arrived = arrived + jnp.where(odd, edge_in[n, 0].astype(f32), edge_in[n, 1].astype(f32))
    rim_out[...] = (border[...] + arrived).astype(bf16)
    to_peers(lambda step: rim(step).start())
    for k in range(last + 1):
        if k >= ahead_of_rim or k in outer:
            to_peers(lambda step: peer(k, step).start())

    def complete(k):
        rim_own = rim_out[...].astype(f32)
        for pair, i, r in rows_of(k):
            own = pr[place[pair], i * tall : (i + 1) * tall, :].astype(f32)
            own = jnp.where(at_ends, pltpu.roll(rim_own, cols - 1 - 2 * r, 1), own)
            misfits[r] = smooth(own - ob[pl.ds(r, tall, stride=pitch), :])
            po[pl.ds(r, tall, stride=pitch), :] = own

    for k in range(last + 1):
        complete(k)

    def pack(o, carry):
        p_ref[o] = po[pl.ds(o * pitch, rows), :].astype(bf16)
        return carry

    lax.fori_loop(0, outputs, pack, 0, unroll=unroll_of(outputs))

    def spread_sum(own, other):
        add = lambda n, run: run + smooth(own - other(n))
        pair_sum = smooth(own - own)
        if members == 2:
            pair_sum = add(0, pair_sum)
        else:
            pair_sum = lax.fori_loop(0, members - 1, add, pair_sum)
        return pair_sum / (members - 1)

    to_peers(lambda step: rim(step).wait())
    rim_own = rim_out[...].astype(f32)
    value = smooth(rim_own - border_obs[...]) - spread_sum(rim_own, lambda n: rim_in[n].astype(f32))
    value = latw[rows : rows + 1, :] * varb[...] * value
    value = jnp.where(odd, pltpu.roll(value, 1, 1), pltpu.roll(value, cols - 1, 1))
    gedge_out[...] = value.astype(bf16)
    for copy in gedges:
        copy.start()
    for copy in gedges:
        copy.wait()
    around[...] = jnp.where(odd, gedge_in[0].astype(f32), gedge_in[1].astype(f32))

    g_rows = row_copies(gs, grow_send, grow_recv)
    ready, done, packed = set(), set(), set()

    def gradient(k):
        to_peers(lambda step: peer(k, step).wait())
        for pair, i, r in rows_of(k):
            at, inside = place[pair], slice(i * tall, (i + 1) * tall)

            def other(n):
                patch = pltpu.roll(rim_in[n].astype(f32), cols - 1 - 2 * r, 1)
                return jnp.where(at_ends, patch, others[n, at, inside, :].astype(f32))

            own = po[pl.ds(r, tall, stride=pitch), :].astype(bf16).astype(f32)
            value = latw[r : r + 1, :] * varb[...] * (misfits[r] - spread_sum(own, other))
            both = pltpu.roll(around[...], cols - 1 - 2 * r, 1)
            ahead = jnp.where(at_last, both, pltpu.roll(value, cols - 1, 1))
            behind = jnp.where(at_first, both, pltpu.roll(value, 1, 1))
            gs[r + 1, 0:tall, :] = ahead.astype(bf16)
            gs[r + 1, padded : padded + tall, :] = value.astype(bf16)
            gs[r + 1, 2 * padded : 2 * padded + tall, :] = behind.astype(bf16)
            ready.add(r)
        if 0 in groups[k]:
            start_up(g_rows)
        if pairs - 1 in groups[k]:
            start_down(g_rows)

    def backward():
        for pair in range(pairs):
            if pair in done or not {2 * pair - 1, 2 * pair, 2 * pair + 1, 2 * pair + 2} <= ready:
                continue
            done.add(pair)
            rhs = jnp.concatenate(
                [gs[2 * pair + i : 2 * pair + i + 3].reshape(9 * padded, cols) for i in range(2)],
                axis=1)
            y = jnp.dot(wb[:, : 9 * padded], rhs, preferred_element_type=f32)
            for i in range(2):
                big[pl.ds(2 * pair + i, channels, stride=pitch), :] = y[:, i * cols : (i + 1) * cols]
        for q in range(chunks):
            if q == chunks // 2 or q in packed or not set(range(q * CHUNK // 2, (q + 1) * CHUNK // 2)) <= done:
                continue
            packed.add(q)

            def narrow(c, carry):
                out_ref[c, q * CHUNK : (q + 1) * CHUNK, :] = (
                    big[pl.ds(c * pitch + q * CHUNK, CHUNK), :].astype(bf16))
                return carry

            lax.fori_loop(0, channels, narrow, 0, unroll=16)

    for k in range(last + 1):
        if k == last - 1 and -1 not in ready and outer[-1] < k:
            wait_rows(g_rows, gs)
            ready.update((-1, rows))
            backward()
        gradient(k)
        backward()
    if -1 not in ready:
        wait_rows(g_rows, gs)
        ready.update((-1, rows))
        backward()


def store(p_ref, slope_ref, big, p_hbm, slope_hbm, tail, sem):
    channels, rows, _ = slope_ref.shape
    pitch, chunks = pitch_of(rows), rows // CHUNK
    middle = chunks // 2 * CHUNK
    above, below = pl.ds(0, middle), pl.ds(middle + CHUNK, rows - middle - CHUNK)
    copies = [pltpu.make_async_copy(p_ref, p_hbm, sem.at[0])]
    for n, part in enumerate((above, below)):
        if part.size:
            copies.append(pltpu.make_async_copy(
                slope_ref.at[:, part, :], slope_hbm.at[:, part, :], sem.at[1 + n]))
    for copy in copies:
        copy.start()
    share = channels // 2
    for h in range(2):

        def narrow(c, carry):
            tail[c] = big[pl.ds(c * pitch + middle, CHUNK), :].astype(bf16)
            return carry

        lax.fori_loop(h * share, (h + 1) * share, narrow, 0, unroll=16)
        part = pl.ds(h * share, share)
        copies.append(pltpu.make_async_copy(
            tail.at[part], slope_hbm.at[part, pl.ds(middle, CHUNK), :], sem.at[3 + h]))
        copies[-1].start()
    for copy in copies:
        copy.wait()


def shards(layer_inputs, conv_weight, channel_offset, observed, var_weight):
    _, channels, rows, cols = layer_inputs.shape
    outputs = conv_weight.shape[2]
    members, lats, lons = [lax.axis_size(n) for n in ("member", "lat", "lon")]
    tall, padded = -(-outputs // 8) * 8, -(-outputs // 16) * 16
    pairs, count = rows // 2, len(plan(rows)[0])
    flat = pltpu.VMEM((tall, cols), f32)
    pitch = pitch_of(rows)
    sizes = (members, lats, lons, channels, rows, cols, outputs, tall, padded)
    held = (outputs + channels) * rows * cols * 2 + channels * pitch * cols * 4 + 65536
    vmem = pl.BlockSpec(memory_space=pltpu.VMEM)
    hbm = pl.BlockSpec(memory_space=pl.ANY)
    dma = pltpu.SemaphoreType.DMA
    wide = -(-9 * padded // 128) * 128
    predicted, slope, wide_slope = pl.pallas_call(
        functools.partial(kernel, sizes),
        out_shape=(
            pltpu.VMEM((outputs, rows, cols), bf16),
            pltpu.VMEM((channels, rows, cols), bf16),
            pltpu.VMEM((channels * pitch, cols), f32),
        ),
        in_specs=[hbm] * 5,
        out_specs=(vmem, vmem, vmem),
        scratch_shapes=[
            pltpu.SMEM(channel_offset.shape, f32),
            pltpu.SMEM(var_weight.shape, f32),
            pltpu.VMEM((channels, rows, cols), bf16),
            pltpu.VMEM(conv_weight.shape, bf16),
            pltpu.VMEM((outputs, rows, cols), bf16),
            dma((rows // TILE + 4,)),
            pltpu.VMEM((rows + 2, channels, cols), bf16),
            pltpu.VMEM((3 * padded, 3 * channels), bf16),
            pltpu.VMEM((wide, channels), bf16),
            pltpu.VMEM((channels, wide), bf16),
            pltpu.VMEM((tall * pitch, cols), f32),
            pltpu.VMEM((pairs, 2 * tall, cols), bf16),
            pltpu.VMEM((members - 1, pairs, 2 * tall, cols), bf16),
            pltpu.VMEM((tall * pitch, cols), f32),
            pltpu.VMEM((rows, tall, cols), f32),
            pltpu.VMEM((rows + 2, 3 * padded, cols), bf16),
            pltpu.VMEM((rows + 8, cols), f32),
            flat, flat, pltpu.VMEM((2, tall, cols), f32), flat, flat, flat,
            pltpu.VMEM((2, tall, cols), bf16),
            pltpu.VMEM((2, 2, tall, cols), bf16),
            pltpu.VMEM((tall, cols), bf16),
            pltpu.VMEM((members - 1, tall, cols), bf16),
            pltpu.VMEM((tall, cols), bf16),
            pltpu.VMEM((2, tall, cols), bf16),
            dma((2,)), dma((2,)), dma((2,)), dma((2,)),
            dma((2, 2)), dma((2, 2)), dma((members - 1,)), dma((members - 1,)), dma((2,)), dma((2,)),
            dma((count, members - 1)), dma((count, members - 1)),
        ],
        compiler_params=pltpu.CompilerParams(
            collective_id=0, has_side_effects=True, vmem_limit_bytes=ROOM - held),
        name="crps_step",
    )(layer_inputs[0], conv_weight, observed, channel_offset, var_weight)
    predicted, slope = pl.pallas_call(
        store,
        out_shape=(
            jax.ShapeDtypeStruct(predicted.shape, bf16),
            jax.ShapeDtypeStruct(slope.shape, bf16),
        ),
        in_specs=[vmem] * 3,
        out_specs=(hbm, hbm),
        scratch_shapes=[pltpu.VMEM((channels, CHUNK, cols), bf16), dma((5,))],
        compiler_params=pltpu.CompilerParams(vmem_limit_bytes=4 * 1024 * 1024),
        name="store",
    )(predicted, slope, wide_slope)
    return predicted[None], slope[None]


def solution(mesh):
    in_specs = (P("member", None, "lat", "lon"), P(), P(), P(None, "lat", "lon"), P())
    out_specs = (P("member", None, "lat", "lon"), P("member", None, "lat", "lon"))
    return jax.shard_map(shards, mesh=mesh, in_specs=in_specs, out_specs=out_specs, check_vma=False)
```

```python
import functools

import jax
import jax.numpy as jnp
from jax import lax
from jax.experimental import pallas as pl
from jax.experimental.pallas import tpu as pltpu
from jax.sharding import PartitionSpec as P

MESH = pl.DeviceIdType.MESH
smoothing = 0.25
CHUNK = 16
TILE = 8
ROOM = 67_043_328
f32, bf16 = jnp.float32, jnp.bfloat16


def smooth(difference):
    return difference * lax.rsqrt(difference * difference + smoothing * smoothing)


def pitch_of(rows):
    return rows + 1 - rows % 2


def plan(rows):
    pairs, half = rows // 2, CHUNK // 2
    chunks = rows // CHUNK
    if chunks < 3:
        return [list(range(1, pairs - 1)), sorted({0, pairs - 1})], 1
    base = chunks // 2 * half
    core = list(range(base + 1, base + half - 1))
    low, high = list(range(1, base + 1)), list(range(base + half - 1, pairs - 1))
    cut = lambda run: [run[max(i - 4, 0) : i] for i in range(len(run), 0, -4)]
    early = [core[:1], core[1:2], core[2:4], low[-4:], low[-8:-4]]
    late = [[0, pairs - 1]] + cut(low[:-8]) + cut(high) + [[pair] for pair in core[4:]]
    return [g for g in early if g] + [g for g in late if g], len([g for g in early if g])


def final_tile(rows):
    return plan(rows)[0][-1][-1] * 2 // TILE


def slope_of(pair, gs, wb):
    _, depth, cols = gs.shape
    rhs = jnp.concatenate(
        [gs[2 * pair + i : 2 * pair + i + 3].reshape(3 * depth, cols) for i in range(2)], axis=1)
    return jnp.dot(wb[:, : 3 * depth], rhs, preferred_element_type=f32)


def kernel(
    sizes,
    x_hbm, w_hbm, obs_hbm, bias_hbm, var_hbm,
    p_ref, out_ref, big, gs, wb,
    bias_ref, var_ref, x_ref, w_ref, obs_ref, load_sem, xt, wf, wbt, po, pr, others,
    ob, misfits, latw, biasb, varb, partial, border, border_obs, around,
    edge_out, edge_in, rim_out, rim_in, gedge_out, gedge_in,
    row_send, row_recv, grow_send, grow_recv,
    edge_send, edge_recv, rim_send, rim_recv, gedge_send, gedge_recv, peer_send, peer_recv,
):
    members, lats, lons, channels, rows, cols, outputs, tall, padded = sizes
    pitch = pitch_of(rows)
    chunks = rows // CHUNK
    pairs = rows // 2
    groups, ahead_of_rim = plan(rows)
    place, first = {}, []
    for group in groups:
        first.append(len(place))
        for pair in group:
            place[pair] = len(place)
    last = len(groups) - 1
    outer = [k for k, group in enumerate(groups) if 0 in group or pairs - 1 in group]
    inner = [k for k in range(last + 1) if k not in outer]
    tiles = rows // TILE
    start = groups[0][0] * 2 // TILE if chunks > 2 else 0
    order = [start, 0, tiles - 1] + [t + start for t in range(1, tiles - start)]
    order = list(dict.fromkeys(order + list(range(start, -1, -1))))
    me, lat, lon = lax.axis_index("member"), lax.axis_index("lat"), lax.axis_index("lon")
    right, left = lax.rem(lon + 1, lons), lax.rem(lon + lons - 1, lons)
    has_up, has_down = lat > 0, lat < lats - 1

    barrier = pltpu.get_barrier_semaphore()

    def greet(step, carry):
        other = lax.rem(me + step, members)
        pl.semaphore_signal(barrier, inc=1, device_id=(other, lat, lon), device_id_type=MESH)
        return carry

    lax.fori_loop(1, members, greet, 0)
    for side in (left, right):
        pl.semaphore_signal(barrier, inc=1, device_id=(me, lat, side), device_id_type=MESH)

    @pl.when(has_up)
    def _():
        pl.semaphore_signal(barrier, inc=1, device_id=(me, lat - 1, lon), device_id_type=MESH)

    @pl.when(has_down)
    def _():
        pl.semaphore_signal(barrier, inc=1, device_id=(me, lat + 1, lon), device_id_type=MESH)

    loads = {"bias": pltpu.make_async_copy(bias_hbm, bias_ref, load_sem.at[tiles + 2])}
    for q in order:
        loads[q] = pltpu.make_async_copy(
            x_hbm.at[:, pl.ds(q * TILE, TILE), :], x_ref.at[:, pl.ds(q * TILE, TILE), :],
            load_sem.at[q])
        if q == start:
            loads["w"] = pltpu.make_async_copy(w_hbm, w_ref, load_sem.at[tiles])
    loads["var"] = pltpu.make_async_copy(var_hbm, var_ref, load_sem.at[tiles + 3])
    loads["obs"] = pltpu.make_async_copy(obs_hbm, obs_ref, load_sem.at[tiles + 1])
    for load in loads.values():
        load.start()

    lane = lax.broadcasted_iota(jnp.int32, (tall, cols), 1)
    at_first, at_last = lane == 0, lane == cols - 1
    at_ends = at_first | at_last
    odd = lane % 2 == 1

    def spread(array, source):
        array[...] = jnp.zeros(array.shape, f32)

        def one(o, carry):
            array[pl.ds(o, 1), :] = jnp.full((1, cols), source[o], f32)
            return carry

        lax.fori_loop(0, outputs, one, 0, unroll=3)

    wf[...] = jnp.zeros(wf.shape, bf16)
    border[...] = jnp.zeros(border.shape, f32)
    loads["bias"].wait()
    spread(biasb, bias_ref)

    def unroll_of(n):
        return max(d for d in range(1, 25) if n % d == 0)

    def turn(r, carry):
        xt[r + 1] = big[pl.ds(r, channels, stride=pitch), :].astype(bf16)
        return carry

    def bring(t):
        loads[t].wait()

        def one(c, carry):
            big[pl.ds(c * pitch + t * TILE, TILE), :] = (
                x_ref[c, t * TILE : (t + 1) * TILE, :].astype(f32))
            return carry

        lax.fori_loop(0, channels, one, 0, unroll=16)
        lax.fori_loop(t * TILE, (t + 1) * TILE, turn, 0, unroll=4)

    def row_copies(array, send, recv):
        up = pltpu.make_async_remote_copy(
            src_ref=array.at[1], dst_ref=array.at[rows + 1], send_sem=send.at[0],
            recv_sem=recv.at[0], device_id=(me, lat - 1, lon), device_id_type=MESH)
        down = pltpu.make_async_remote_copy(
            src_ref=array.at[rows], dst_ref=array.at[0], send_sem=send.at[1],
            recv_sem=recv.at[1], device_id=(me, lat + 1, lon), device_id_type=MESH)
        return up, down

    def start_up(copies):
        pl.when(has_up)(lambda: copies[0].start())

    def start_down(copies):
        pl.when(has_down)(lambda: copies[1].start())

    def wait_rows(copies, array):
        @pl.when(has_up)
        def _():
            copies[1].wait_recv()
            copies[0].wait_send()

        @pl.when(has_down)
        def _():
            copies[0].wait_recv()
            copies[1].wait_send()

        @pl.when(lat == 0)
        def _():
            array[0] = jnp.zeros(array.shape[1:], bf16)

        @pl.when(lat == lats - 1)
        def _():
            array[rows + 1] = jnp.zeros(array.shape[1:], bf16)

    def edge_copies(source, target, send, recv):
        return [
            pltpu.make_async_remote_copy(
                src_ref=source, dst_ref=target.at[s], send_sem=send.at[s],
                recv_sem=recv.at[s], device_id=(me, lat, side), device_id_type=MESH)
            for s, side in enumerate((right, left))]

    def to_peers(act):
        def one(step, carry):
            act(step)
            return carry

        lax.fori_loop(1, members, one, 0)

    peer = lambda k, step: pltpu.make_async_remote_copy(
        src_ref=pr.at[pl.ds(first[k], len(groups[k]))],
        dst_ref=others.at[step - 1, pl.ds(first[k], len(groups[k]))],
        send_sem=peer_send.at[k, step - 1], recv_sem=peer_recv.at[k, step - 1],
        device_id=(lax.rem(me + step, members), lat, lon), device_id_type=MESH)
    rim = lambda step: pltpu.make_async_remote_copy(
        src_ref=rim_out, dst_ref=rim_in.at[step - 1],
        send_sem=rim_send.at[step - 1], recv_sem=rim_recv.at[step - 1],
        device_id=(lax.rem(me + step, members), lat, lon), device_id_type=MESH)
    edges = [
        edge_copies(edge_out.at[n], edge_in.at[n], edge_send.at[n], edge_recv.at[n])
        for n in range(2)]
    gedges = edge_copies(gedge_out, gedge_in, gedge_send, gedge_recv)

    def rows_of(k):
        return [(pair, i, 2 * pair + i) for pair in groups[k] for i in range(2)]

    def forward(k):
        share = jnp.zeros((tall, cols), f32)
        own = jnp.zeros((tall, cols), f32)
        for pair in groups[k]:
            rhs = jnp.concatenate(
                [xt[2 * pair + i : 2 * pair + i + 3].reshape(3 * channels, cols) for i in range(2)],
                axis=1)
            y = jnp.dot(wf[...], rhs, preferred_element_type=f32)
            for i in range(2):
                r = 2 * pair + i
                from_left, mid, from_right = [
                    y[b * padded : b * padded + tall, i * cols : (i + 1) * cols] for b in range(3)]
                from_left = pltpu.roll(from_left, 1, 1)
                from_right = pltpu.roll(from_right, cols - 1, 1)
                total = mid + biasb[...] + jnp.where(at_first, 0.0, from_left)
                total = total + jnp.where(at_last, 0.0, from_right)
                pr[place[pair], i * tall : (i + 1) * tall, :] = total.astype(bf16)
                both = pltpu.roll(jnp.where(at_first, from_left, from_right), 2 * r + 1, 1)
                mine = lane // 2 == r
                share = jnp.where(mine, both, share)
                own = jnp.where(mine, pltpu.roll(total, 2 * r + 1, 1), own)
        at = 1 if k in outer else 0
        partial[at] = share if k in (outer[0], inner[0]) else partial[at] + share
        border[...] = border[...] + own

    def exchange(n):
        edge_out[n] = partial[n].astype(bf16)
        for copy in edges[n]:
            copy.start()

    def enter():
        pl.semaphore_wait(barrier, members + 1 + has_up.astype(jnp.int32) + has_down.astype(jnp.int32))

    x_rows = row_copies(xt, row_send, row_recv)
    waiting = list(order)
    bring(waiting.pop(0))
    loads["w"].wait()
    for a in range(3):
        for b in range(3):
            wf[b * padded : b * padded + outputs, a * channels : (a + 1) * channels] = w_ref[a, b]
    for n, k in enumerate(inner):
        needed = {r // TILE for pair in groups[k] for r in range(2 * pair - 1, 2 * pair + 3)}
        while needed & set(waiting):
            bring(waiting.pop(0))
        forward(k)
        if n == 0:
            enter()
        if k < ahead_of_rim:
            to_peers(lambda step: peer(k, step).start())
        if n == min(1, len(inner) - 1):
            while {0, tiles - 1} & set(waiting):
                bring(waiting.pop(0))
            start_up(x_rows)
            start_down(x_rows)
    exchange(0)

    border_obs[...] = jnp.zeros(border_obs.shape, f32)
    loads["var"].wait()
    spread(varb, var_ref)

    def blank(r, carry):
        for b in range(3):
            gs[r, b * padded + tall : (b + 1) * padded, :] = jnp.zeros((padded - tall, cols), bf16)
        return carry

    lax.fori_loop(1, rows + 1, blank, 0)
    loads["obs"].wait()

    def widen_obs(o, carry):
        ob[pl.ds(o * pitch, rows), :] = obs_ref[o].astype(f32)
        return carry

    lax.fori_loop(0, outputs, widen_obs, 0, unroll=unroll_of(outputs))
    ob[pl.ds(outputs * pitch, (tall - outputs) * pitch), :] = jnp.zeros(
        ((tall - outputs) * pitch, cols), f32)
    wait_rows(x_rows, xt)
    for k in outer:
        forward(k)
    exchange(1)

    wbt[...] = jnp.zeros(wbt.shape, bf16)
    for a in range(3):
        for b in range(3):
            base = ((2 - a) * 3 + b) * padded
            wbt[base : base + outputs, :] = w_ref[a, b]
    wb[...] = jnp.transpose(wbt[...])

    def latitude(row):
        row_index = (lat * rows + row).astype(f32)
        return jnp.cos((-80.0 + 160.0 * (row_index + 0.5) / float(rows * lats)) * (jnp.pi / 180.0))

    latw[0:rows, :] = latitude(lax.broadcasted_iota(jnp.int32, (rows, cols), 0))
    latw[rows : rows + 8, :] = latitude(lax.broadcasted_iota(jnp.int32, (8, cols), 1) // 2)

    def gather_obs(k):
        own = jnp.zeros((tall, cols), f32)
        for _, _, r in rows_of(k):
            turned = pltpu.roll(ob[pl.ds(r, tall, stride=pitch), :], 2 * r + 1, 1)
            own = jnp.where(lane // 2 == r, turned, own)
        border_obs[...] = border_obs[...] + own

    for k in range(last + 1):
        gather_obs(k)

    arrived = jnp.zeros((tall, cols), f32)
    for n in range(2):
        for copy in edges[n]:
            copy.wait()
        arrived = arrived + jnp.where(odd, edge_in[n, 0].astype(f32), edge_in[n, 1].astype(f32))
    rim_out[...] = (border[...] + arrived).astype(bf16)
    to_peers(lambda step: rim(step).start())
    for k in range(last + 1):
        if k >= ahead_of_rim or k in outer:
            to_peers(lambda step: peer(k, step).start())

    def complete(k):
        rim_own = rim_out[...].astype(f32)
        for pair, i, r in rows_of(k):
            own = pr[place[pair], i * tall : (i + 1) * tall, :].astype(f32)
            own = jnp.where(at_ends, pltpu.roll(rim_own, cols - 1 - 2 * r, 1), own)
            misfits[r] = smooth(own - ob[pl.ds(r, tall, stride=pitch), :])
            po[pl.ds(r, tall, stride=pitch), :] = own

    for k in range(last + 1):
        complete(k)

    def pack(o, carry):
        p_ref[o] = po[pl.ds(o * pitch, rows), :].astype(bf16)
        return carry

    lax.fori_loop(0, outputs, pack, 0, unroll=unroll_of(outputs))

    def spread_sum(own, other):
        add = lambda n, run: run + smooth(own - other(n))
        pair_sum = smooth(own - own)
        if members == 2:
            pair_sum = add(0, pair_sum)
        else:
            pair_sum = lax.fori_loop(0, members - 1, add, pair_sum)
        return pair_sum / (members - 1)

    to_peers(lambda step: rim(step).wait())
    rim_own = rim_out[...].astype(f32)
    value = smooth(rim_own - border_obs[...]) - spread_sum(rim_own, lambda n: rim_in[n].astype(f32))
    value = latw[rows : rows + 1, :] * varb[...] * value
    value = jnp.where(odd, pltpu.roll(value, 1, 1), pltpu.roll(value, cols - 1, 1))
    gedge_out[...] = value.astype(bf16)
    for copy in gedges:
        copy.start()
    for copy in gedges:
        copy.wait()
    around[...] = jnp.where(odd, gedge_in[0], gedge_in[1])

    g_rows = row_copies(gs, grow_send, grow_recv)
    ready, done, packed = set(), set(), set()
    left_over = [final_tile(rows) * TILE // 2 + n for n in range(TILE // 2)]

    def gradient(k):
        to_peers(lambda step: peer(k, step).wait())
        for pair, i, r in rows_of(k):
            at, inside = place[pair], slice(i * tall, (i + 1) * tall)

            def other(n):
                patch = pltpu.roll(rim_in[n], cols - 1 - 2 * r, 1)
                return jnp.where(at_ends, patch, others[n, at, inside, :]).astype(f32)

            own = po[pl.ds(r, tall, stride=pitch), :].astype(bf16).astype(f32)
            value = latw[r : r + 1, :] * varb[...] * (misfits[r] - spread_sum(own, other))
            value = value.astype(bf16)
            both = pltpu.roll(around[...], cols - 1 - 2 * r, 1)
            gs[r + 1, 0:tall, :] = jnp.where(at_last, both, pltpu.roll(value, cols - 1, 1))
            gs[r + 1, padded : padded + tall, :] = value
            gs[r + 1, 2 * padded : 2 * padded + tall, :] = jnp.where(
                at_first, both, pltpu.roll(value, 1, 1))
            ready.add(r)
        if 0 in groups[k]:
            start_up(g_rows)
        if pairs - 1 in groups[k]:
            start_down(g_rows)

    def backward():
        for pair in range(pairs):
            if pair in left_over or pair in done or not {2 * pair - 1, 2 * pair, 2 * pair + 1, 2 * pair + 2} <= ready:
                continue
            done.add(pair)
            y = slope_of(pair, gs, wb)
            for i in range(2):
                big[pl.ds(2 * pair + i, channels, stride=pitch), :] = y[:, i * cols : (i + 1) * cols]
        for q in range(chunks):
            if q == final_tile(rows) * TILE // CHUNK or q in packed or not set(range(q * CHUNK // 2, (q + 1) * CHUNK // 2)) <= done:
                continue
            packed.add(q)

            def narrow(c, carry):
                out_ref[c, q * CHUNK : (q + 1) * CHUNK, :] = (
                    big[pl.ds(c * pitch + q * CHUNK, CHUNK), :].astype(bf16))
                return carry

            lax.fori_loop(0, channels, narrow, 0, unroll=16)

    sequence = outer + inner
    for k in sequence:
        if k == sequence[-2] and k not in outer:
            wait_rows(g_rows, gs)
            ready.update((-1, rows))
            backward()
        gradient(k)
        backward()
    if -1 not in ready:
        wait_rows(g_rows, gs)
        ready.update((-1, rows))
        backward()


def store(p_ref, slope_ref, big, gs, wb, p_hbm, slope_hbm, last_rows, tail, sem):
    channels, rows, cols = slope_ref.shape
    pitch, short = pitch_of(rows), pitch_of(TILE)
    tile = final_tile(rows)
    chunk = tile * TILE // CHUNK * CHUNK
    above, below = pl.ds(0, chunk), pl.ds(chunk + CHUNK, rows - chunk - CHUNK)
    copies = [pltpu.make_async_copy(p_ref, p_hbm, sem.at[0])]
    for n, part in enumerate((above, below)):
        if part.size:
            copies.append(pltpu.make_async_copy(
                slope_ref.at[:, part, :], slope_hbm.at[:, part, :], sem.at[1 + n]))
    for copy in copies:
        copy.start()

    def send(n, t, source, stride, start):
        def narrow(c, carry):
            tail[n, c] = source[pl.ds(c * stride + start, TILE), :].astype(bf16)
            return carry

        lax.fori_loop(0, channels, narrow, 0, unroll=16)
        copies.append(pltpu.make_async_copy(
            tail.at[n], slope_hbm.at[:, pl.ds(t * TILE, TILE), :], sem.at[3 + n]))
        copies[-1].start()

    beside = tile + 1 - tile % 2 * 2
    send(0, beside, big, pitch, beside * TILE)
    for n in range(TILE // 2):
        y = slope_of(tile * TILE // 2 + n, gs, wb)
        for i in range(2):
            last_rows[pl.ds(2 * n + i, channels, stride=short), :] = y[:, i * cols : (i + 1) * cols]
    send(1, tile, last_rows, short, 0)
    for copy in copies:
        copy.wait()


def shards(layer_inputs, conv_weight, channel_offset, observed, var_weight):
    _, channels, rows, cols = layer_inputs.shape
    outputs = conv_weight.shape[2]
    members, lats, lons = [lax.axis_size(n) for n in ("member", "lat", "lon")]
    tall, padded = -(-outputs // 8) * 8, -(-outputs // 16) * 16
    pairs, count = rows // 2, len(plan(rows)[0])
    flat = pltpu.VMEM((tall, cols), f32)
    pitch = pitch_of(rows)
    sizes = (members, lats, lons, channels, rows, cols, outputs, tall, padded)
    vmem = pl.BlockSpec(memory_space=pltpu.VMEM)
    hbm = pl.BlockSpec(memory_space=pl.ANY)
    dma = pltpu.SemaphoreType.DMA
    wide = -(-9 * padded // 128) * 128
    held = (outputs + channels) * rows * cols * 2 + channels * pitch * cols * 4 + 65536
    held += (rows + 2) * 3 * padded * cols * 2 + channels * wide * 2
    predicted, slope, *parts = pl.pallas_call(
        functools.partial(kernel, sizes),
        out_shape=(
            pltpu.VMEM((outputs, rows, cols), bf16),
            pltpu.VMEM((channels, rows, cols), bf16),
            pltpu.VMEM((channels * pitch, cols), f32),
            pltpu.VMEM((rows + 2, 3 * padded, cols), bf16),
            pltpu.VMEM((channels, wide), bf16),
        ),
        in_specs=[hbm] * 5,
        out_specs=(vmem,) * 5,
        scratch_shapes=[
            pltpu.SMEM(channel_offset.shape, f32),
            pltpu.SMEM(var_weight.shape, f32),
            pltpu.VMEM((channels, rows, cols), bf16),
            pltpu.VMEM(conv_weight.shape, bf16),
            pltpu.VMEM((outputs, rows, cols), bf16),
            dma((rows // TILE + 4,)),
            pltpu.VMEM((rows + 2, channels, cols), bf16),
            pltpu.VMEM((3 * padded, 3 * channels), bf16),
            pltpu.VMEM((wide, channels), bf16),
            pltpu.VMEM((tall * pitch, cols), f32),
            pltpu.VMEM((pairs, 2 * tall, cols), bf16),
            pltpu.VMEM((members - 1, pairs, 2 * tall, cols), bf16),
            pltpu.VMEM((tall * pitch, cols), f32),
            pltpu.VMEM((rows, tall, cols), f32),
            pltpu.VMEM((rows + 8, cols), f32),
            flat, flat, pltpu.VMEM((2, tall, cols), f32), flat, flat, pltpu.VMEM((tall, cols), bf16),
            pltpu.VMEM((2, tall, cols), bf16),
            pltpu.VMEM((2, 2, tall, cols), bf16),
            pltpu.VMEM((tall, cols), bf16),
            pltpu.VMEM((members - 1, tall, cols), bf16),
            pltpu.VMEM((tall, cols), bf16),
            pltpu.VMEM((2, tall, cols), bf16),
            dma((2,)), dma((2,)), dma((2,)), dma((2,)),
            dma((2, 2)), dma((2, 2)), dma((members - 1,)), dma((members - 1,)), dma((2,)), dma((2,)),
            dma((count, members - 1)), dma((count, members - 1)),
        ],
        compiler_params=pltpu.CompilerParams(
            collective_id=0, has_side_effects=True, vmem_limit_bytes=ROOM - held),
        name="crps_step",
    )(layer_inputs[0], conv_weight, observed, channel_offset, var_weight)
    predicted, slope = pl.pallas_call(
        store,
        out_shape=(
            jax.ShapeDtypeStruct(predicted.shape, bf16),
            jax.ShapeDtypeStruct(slope.shape, bf16),
        ),
        in_specs=[vmem] * 5,
        out_specs=(hbm, hbm),
        scratch_shapes=[
            pltpu.VMEM((channels * pitch_of(TILE), cols), f32),
            pltpu.VMEM((2, channels, TILE, cols), bf16),
            dma((5,)),
        ],
        compiler_params=pltpu.CompilerParams(vmem_limit_bytes=8 * 1024 * 1024),
        name="store",
    )(predicted, slope, *parts)
    return predicted[None], slope[None]


def solution(mesh):
    in_specs = (P("member", None, "lat", "lon"), P(), P(), P(None, "lat", "lon"), P())
    out_specs = (P("member", None, "lat", "lon"), P("member", None, "lat", "lon"))
    return jax.shard_map(shards, mesh=mesh, in_specs=in_specs, out_specs=out_specs, check_vma=False)
```

```python
import functools

import jax
import jax.numpy as jnp
from jax import lax
from jax.experimental import pallas as pl
from jax.experimental.pallas import tpu as pltpu
from jax.sharding import PartitionSpec as P

MESH = pl.DeviceIdType.MESH
smoothing = 0.25
CHUNK = 16
TILE = 8
ROOM = 67_043_328
f32, bf16 = jnp.float32, jnp.bfloat16


def smooth(difference):
    return difference * lax.rsqrt(difference * difference + smoothing * smoothing)


def pitch_of(rows):
    return rows + 1 - rows % 2


def plan(rows):
    pairs, half = rows // 2, CHUNK // 2
    chunks = rows // CHUNK
    if chunks < 3:
        return [list(range(1, pairs - 1)), sorted({0, pairs - 1})], 1
    base = chunks // 2 * half
    core = list(range(base + 1, base + half - 1))
    low, high = list(range(1, base + 1)), list(range(base + half - 1, pairs - 1))
    cut = lambda run: [run[max(i - 4, 0) : i] for i in range(len(run), 0, -4)]
    early = [core[:1], core[1:2], core[2:4], low[-4:], low[-8:-4]]
    late = [[0, pairs - 1]] + cut(low[:-8]) + cut(high) + [[pair] for pair in core[4:]]
    return [g for g in early if g] + [g for g in late if g], len([g for g in early if g])


def spans(rows, outputs):
    sizes = [-(-2 * len(group) * outputs // 8) * 8 for group in plan(rows)[0]]
    return [sum(sizes[:k]) for k in range(len(sizes))], sizes


def final_tile(rows):
    return plan(rows)[0][-1][-1] * 2 // TILE


def slope_of(pair, gs, wb):
    _, depth, cols = gs.shape
    rhs = jnp.concatenate(
        [gs[2 * pair + i : 2 * pair + i + 3].reshape(3 * depth, cols) for i in range(2)], axis=1)
    return jnp.dot(wb[:, : 3 * depth], rhs, preferred_element_type=f32)


def kernel(
    sizes,
    x_hbm, w_hbm, obs_hbm, bias_hbm, var_hbm,
    p_ref, out_ref, big, gs, wb,
    bias_ref, var_ref, x_ref, w_ref, obs_ref, load_sem, xt, wf, wbt, po, pr, stage, others, spare,
    ob, misfits, latw, biasb, varb, partial, border, border_obs, around,
    edge_out, edge_in, rim_out, rim_in, gedge_out, gedge_in,
    row_send, row_recv, grow_send, grow_recv,
    edge_send, edge_recv, rim_send, rim_recv, gedge_send, gedge_recv, peer_send, peer_recv,
):
    members, lats, lons, channels, rows, cols, outputs, tall, padded = sizes
    pitch = pitch_of(rows)
    chunks = rows // CHUNK
    pairs = rows // 2
    groups, ahead_of_rim = plan(rows)
    first, length = spans(rows, outputs)
    last = len(groups) - 1
    outer = [k for k, group in enumerate(groups) if 0 in group or pairs - 1 in group]
    inner = [k for k in range(last + 1) if k not in outer]
    tiles = rows // TILE
    start = groups[0][0] * 2 // TILE if chunks > 2 else 0
    order = [start, 0, tiles - 1] + [t + start for t in range(1, tiles - start)]
    order = list(dict.fromkeys(order + list(range(start, -1, -1))))
    me, lat, lon = lax.axis_index("member"), lax.axis_index("lat"), lax.axis_index("lon")
    right, left = lax.rem(lon + 1, lons), lax.rem(lon + lons - 1, lons)
    has_up, has_down = lat > 0, lat < lats - 1

    barrier = pltpu.get_barrier_semaphore()

    def greet(step, carry):
        other = lax.rem(me + step, members)
        pl.semaphore_signal(barrier, inc=1, device_id=(other, lat, lon), device_id_type=MESH)
        return carry

    lax.fori_loop(1, members, greet, 0)
    for side in (left, right):
        pl.semaphore_signal(barrier, inc=1, device_id=(me, lat, side), device_id_type=MESH)

    @pl.when(has_up)
    def _():
        pl.semaphore_signal(barrier, inc=1, device_id=(me, lat - 1, lon), device_id_type=MESH)

    @pl.when(has_down)
    def _():
        pl.semaphore_signal(barrier, inc=1, device_id=(me, lat + 1, lon), device_id_type=MESH)

    loads = {"bias": pltpu.make_async_copy(bias_hbm, bias_ref, load_sem.at[tiles + 2])}
    for q in order:
        loads[q] = pltpu.make_async_copy(
            x_hbm.at[:, pl.ds(q * TILE, TILE), :], x_ref.at[:, pl.ds(q * TILE, TILE), :],
            load_sem.at[q])
        if q == start:
            loads["w"] = pltpu.make_async_copy(w_hbm, w_ref, load_sem.at[tiles])
    loads["var"] = pltpu.make_async_copy(var_hbm, var_ref, load_sem.at[tiles + 3])
    loads["obs"] = pltpu.make_async_copy(obs_hbm, obs_ref, load_sem.at[tiles + 1])
    for load in loads.values():
        load.start()

    lane = lax.broadcasted_iota(jnp.int32, (tall, cols), 1)
    at_first, at_last = lane == 0, lane == cols - 1
    at_ends = at_first | at_last
    odd = lane % 2 == 1

    def spread(array, source):
        array[...] = jnp.zeros(array.shape, f32)

        def one(o, carry):
            array[pl.ds(o, 1), :] = jnp.full((1, cols), source[o], f32)
            return carry

        lax.fori_loop(0, outputs, one, 0, unroll=3)

    wf[...] = jnp.zeros(wf.shape, bf16)
    border[...] = jnp.zeros(border.shape, f32)
    loads["bias"].wait()
    spread(biasb, bias_ref)

    def unroll_of(n):
        return max(d for d in range(1, 25) if n % d == 0)

    def turn(r, carry):
        xt[r + 1] = big[pl.ds(r, channels, stride=pitch), :].astype(bf16)
        return carry

    def bring(t):
        loads[t].wait()

        def one(c, carry):
            big[pl.ds(c * pitch + t * TILE, TILE), :] = (
                x_ref[c, t * TILE : (t + 1) * TILE, :].astype(f32))
            return carry

        lax.fori_loop(0, channels, one, 0, unroll=16)
        lax.fori_loop(t * TILE, (t + 1) * TILE, turn, 0, unroll=4)

    def row_copies(array, send, recv):
        up = pltpu.make_async_remote_copy(
            src_ref=array.at[1], dst_ref=array.at[rows + 1], send_sem=send.at[0],
            recv_sem=recv.at[0], device_id=(me, lat - 1, lon), device_id_type=MESH)
        down = pltpu.make_async_remote_copy(
            src_ref=array.at[rows], dst_ref=array.at[0], send_sem=send.at[1],
            recv_sem=recv.at[1], device_id=(me, lat + 1, lon), device_id_type=MESH)
        return up, down

    def start_up(copies):
        pl.when(has_up)(lambda: copies[0].start())

    def start_down(copies):
        pl.when(has_down)(lambda: copies[1].start())

    def wait_rows(copies, array):
        @pl.when(has_up)
        def _():
            copies[1].wait_recv()
            copies[0].wait_send()

        @pl.when(has_down)
        def _():
            copies[0].wait_recv()
            copies[1].wait_send()

        @pl.when(lat == 0)
        def _():
            array[0] = jnp.zeros(array.shape[1:], bf16)

        @pl.when(lat == lats - 1)
        def _():
            array[rows + 1] = jnp.zeros(array.shape[1:], bf16)

    def edge_copies(source, target, send, recv):
        return [
            pltpu.make_async_remote_copy(
                src_ref=source, dst_ref=target.at[s], send_sem=send.at[s],
                recv_sem=recv.at[s], device_id=(me, lat, side), device_id_type=MESH)
            for s, side in enumerate((right, left))]

    def to_peers(act):
        def one(step, carry):
            act(step)
            return carry

        lax.fori_loop(1, members, one, 0)

    peer = lambda k, step: pltpu.make_async_remote_copy(
        src_ref=pr.at[pl.ds(first[k], length[k])],
        dst_ref=others.at[step - 1, pl.ds(first[k], length[k])],
        send_sem=peer_send.at[k, step - 1], recv_sem=peer_recv.at[k, step - 1],
        device_id=(lax.rem(me + step, members), lat, lon), device_id_type=MESH)
    rim = lambda step: pltpu.make_async_remote_copy(
        src_ref=rim_out, dst_ref=rim_in.at[step - 1],
        send_sem=rim_send.at[step - 1], recv_sem=rim_recv.at[step - 1],
        device_id=(lax.rem(me + step, members), lat, lon), device_id_type=MESH)
    edges = [
        edge_copies(edge_out.at[n], edge_in.at[n], edge_send.at[n], edge_recv.at[n])
        for n in range(2)]
    gedges = edge_copies(gedge_out, gedge_in, gedge_send, gedge_recv)

    def rows_of(k):
        return [(pair, i, 2 * pair + i) for pair in groups[k] for i in range(2)]

    def forward(k):
        share = jnp.zeros((tall, cols), f32)
        own = jnp.zeros((tall, cols), f32)
        for j, pair in enumerate(groups[k]):
            rhs = jnp.concatenate(
                [xt[2 * pair + i : 2 * pair + i + 3].reshape(3 * channels, cols) for i in range(2)],
                axis=1)
            y = jnp.dot(wf[...], rhs, preferred_element_type=f32)
            for i in range(2):
                r = 2 * pair + i
                from_left, mid, from_right = [
                    y[b * padded : b * padded + tall, i * cols : (i + 1) * cols] for b in range(3)]
                from_left = pltpu.roll(from_left, 1, 1)
                from_right = pltpu.roll(from_right, cols - 1, 1)
                total = mid + biasb[...] + jnp.where(at_first, 0.0, from_left)
                total = total + jnp.where(at_last, 0.0, from_right)
                po[pl.ds(r, tall, stride=pitch), :] = total
                at = (2 * j + i) * outputs
                stage[at : at + tall, :] = total
                both = pltpu.roll(jnp.where(at_first, from_left, from_right), 2 * r + 1, 1)
                mine = lane // 2 == r
                share = jnp.where(mine, both, share)
                own = jnp.where(mine, pltpu.roll(total, 2 * r + 1, 1), own)
        pr[first[k] : first[k] + length[k], :] = stage[0 : length[k], :].astype(bf16)
        at = 1 if k in outer else 0
        partial[at] = share if k in (outer[0], inner[0]) else partial[at] + share
        border[...] = border[...] + own

    def exchange(n):
        edge_out[n] = partial[n].astype(bf16)
        for copy in edges[n]:
            copy.start()

    def enter():
        pl.semaphore_wait(barrier, members + 1 + has_up.astype(jnp.int32) + has_down.astype(jnp.int32))

    x_rows = row_copies(xt, row_send, row_recv)
    waiting = list(order)
    bring(waiting.pop(0))
    loads["w"].wait()
    for a in range(3):
        for b in range(3):
            wf[b * padded : b * padded + outputs, a * channels : (a + 1) * channels] = w_ref[a, b]
    for n, k in enumerate(inner):
        needed = {r // TILE for pair in groups[k] for r in range(2 * pair - 1, 2 * pair + 3)}
        while needed & set(waiting):
            bring(waiting.pop(0))
        forward(k)
        if n == 0:
            enter()
        if k < ahead_of_rim:
            to_peers(lambda step: peer(k, step).start())
        if n == min(1, len(inner) - 1):
            while {0, tiles - 1} & set(waiting):
                bring(waiting.pop(0))
            start_up(x_rows)
            start_down(x_rows)
    exchange(0)

    border_obs[...] = jnp.zeros(border_obs.shape, f32)
    loads["var"].wait()
    spread(varb, var_ref)

    def blank(r, carry):
        for b in range(3):
            gs[r, b * padded + tall : (b + 1) * padded, :] = jnp.zeros((padded - tall, cols), bf16)
        return carry

    lax.fori_loop(1, rows + 1, blank, 0)
    loads["obs"].wait()

    def widen_obs(o, carry):
        ob[pl.ds(o * pitch, rows), :] = obs_ref[o].astype(f32)
        return carry

    lax.fori_loop(0, outputs, widen_obs, 0, unroll=unroll_of(outputs))
    ob[pl.ds(outputs * pitch, (tall - outputs) * pitch), :] = jnp.zeros(
        ((tall - outputs) * pitch, cols), f32)
    wait_rows(x_rows, xt)
    for k in outer:
        forward(k)
    exchange(1)

    wbt[...] = jnp.zeros(wbt.shape, bf16)
    for a in range(3):
        for b in range(3):
            base = ((2 - a) * 3 + b) * padded
            wbt[base : base + outputs, :] = w_ref[a, b]
    wb[...] = jnp.transpose(wbt[...])

    def latitude(row):
        row_index = (lat * rows + row).astype(f32)
        return jnp.cos((-80.0 + 160.0 * (row_index + 0.5) / float(rows * lats)) * (jnp.pi / 180.0))

    latw[0:rows, :] = latitude(lax.broadcasted_iota(jnp.int32, (rows, cols), 0))
    latw[rows : rows + 8, :] = latitude(lax.broadcasted_iota(jnp.int32, (8, cols), 1) // 2)

    def gather_obs(k):
        own = jnp.zeros((tall, cols), f32)
        for _, _, r in rows_of(k):
            turned = pltpu.roll(ob[pl.ds(r, tall, stride=pitch), :], 2 * r + 1, 1)
            own = jnp.where(lane // 2 == r, turned, own)
        border_obs[...] = border_obs[...] + own

    for k in range(last + 1):
        gather_obs(k)

    arrived = jnp.zeros((tall, cols), f32)
    for n in range(2):
        for copy in edges[n]:
            copy.wait()
        arrived = arrived + jnp.where(odd, edge_in[n, 0].astype(f32), edge_in[n, 1].astype(f32))
    rim_out[...] = (border[...] + arrived).astype(bf16)
    to_peers(lambda step: rim(step).start())
    for k in range(last + 1):
        if k >= ahead_of_rim or k in outer:
            to_peers(lambda step: peer(k, step).start())

    def complete(k):
        rim_own = rim_out[...].astype(f32)
        for pair, i, r in rows_of(k):
            own = po[pl.ds(r, tall, stride=pitch), :]
            own = jnp.where(at_ends, pltpu.roll(rim_own, cols - 1 - 2 * r, 1), own)
            own = own.astype(bf16).astype(f32)
            misfits[r] = smooth(own - ob[pl.ds(r, tall, stride=pitch), :])
            po[pl.ds(r, tall, stride=pitch), :] = own

    for k in range(last + 1):
        complete(k)

    def pack(o, carry):
        p_ref[o] = po[pl.ds(o * pitch, rows), :].astype(bf16)
        return carry

    lax.fori_loop(0, outputs, pack, 0, unroll=unroll_of(outputs))

    def spread_sum(own, other):
        add = lambda n, run: run + smooth(own - other(n))
        pair_sum = smooth(own - own)
        if members == 2:
            pair_sum = add(0, pair_sum)
        else:
            pair_sum = lax.fori_loop(0, members - 1, add, pair_sum)
        return pair_sum / (members - 1)

    to_peers(lambda step: rim(step).wait())
    rim_own = rim_out[...].astype(f32)
    value = smooth(rim_own - border_obs[...]) - spread_sum(rim_own, lambda n: rim_in[n].astype(f32))
    value = latw[rows : rows + 1, :] * varb[...] * value
    value = jnp.where(odd, pltpu.roll(value, 1, 1), pltpu.roll(value, cols - 1, 1))
    gedge_out[...] = value.astype(bf16)
    for copy in gedges:
        copy.start()
    for copy in gedges:
        copy.wait()
    around[...] = jnp.where(odd, gedge_in[0], gedge_in[1])

    g_rows = row_copies(gs, grow_send, grow_recv)
    ready, done, packed = set(), set(), set()
    left_over = [final_tile(rows) * TILE // 2 + n for n in range(TILE // 2)]

    def gradient(k):
        to_peers(lambda step: peer(k, step).wait())

        def unfold(n, carry):
            spare[n, 0 : length[k], :] = others[n, first[k] : first[k] + length[k], :].astype(f32)
            spare[n, length[k] : length[k] + 8, :] = jnp.zeros((8, cols), f32)
            return carry

        lax.fori_loop(0, members - 1, unfold, 0)
        for j, (_, _, r) in enumerate(rows_of(k)):

            def other(n):
                patch = pltpu.roll(rim_in[n], cols - 1 - 2 * r, 1)
                theirs = spare[n, j * outputs : j * outputs + tall, :]
                return jnp.where(at_ends, patch.astype(f32), theirs)

            own = po[pl.ds(r, tall, stride=pitch), :]
            value = latw[r : r + 1, :] * varb[...] * (misfits[r] - spread_sum(own, other))
            value = value.astype(bf16)
            both = pltpu.roll(around[...], cols - 1 - 2 * r, 1)
            gs[r + 1, 0:tall, :] = jnp.where(at_last, both, pltpu.roll(value, cols - 1, 1))
            gs[r + 1, padded : padded + tall, :] = value
            gs[r + 1, 2 * padded : 2 * padded + tall, :] = jnp.where(
                at_first, both, pltpu.roll(value, 1, 1))
            ready.add(r)
        if 0 in groups[k]:
            start_up(g_rows)
        if pairs - 1 in groups[k]:
            start_down(g_rows)

    def backward():
        for pair in range(pairs):
            if pair in left_over or pair in done or not {2 * pair - 1, 2 * pair, 2 * pair + 1, 2 * pair + 2} <= ready:
                continue
            done.add(pair)
            y = slope_of(pair, gs, wb)
            for i in range(2):
                big[pl.ds(2 * pair + i, channels, stride=pitch), :] = y[:, i * cols : (i + 1) * cols]
        for q in range(chunks):
            if q == final_tile(rows) * TILE // CHUNK or q in packed or not set(range(q * CHUNK // 2, (q + 1) * CHUNK // 2)) <= done:
                continue
            packed.add(q)

            def narrow(c, carry):
                out_ref[c, q * CHUNK : (q + 1) * CHUNK, :] = (
                    big[pl.ds(c * pitch + q * CHUNK, CHUNK), :].astype(bf16))
                return carry

            lax.fori_loop(0, channels, narrow, 0, unroll=16)

    sequence = outer + inner
    for k in sequence:
        if k == sequence[-2] and k not in outer:
            wait_rows(g_rows, gs)
            ready.update((-1, rows))
            backward()
        gradient(k)
        backward()
    if -1 not in ready:
        wait_rows(g_rows, gs)
        ready.update((-1, rows))
        backward()


def store(p_ref, slope_ref, big, gs, wb, p_hbm, slope_hbm, last_rows, tail, sem):
    channels, rows, cols = slope_ref.shape
    pitch, short = pitch_of(rows), pitch_of(TILE)
    tile = final_tile(rows)
    chunk = tile * TILE // CHUNK * CHUNK
    above, below = pl.ds(0, chunk), pl.ds(chunk + CHUNK, rows - chunk - CHUNK)
    copies = [pltpu.make_async_copy(p_ref, p_hbm, sem.at[0])]
    for n, part in enumerate((above, below)):
        if part.size:
            copies.append(pltpu.make_async_copy(
                slope_ref.at[:, part, :], slope_hbm.at[:, part, :], sem.at[1 + n]))
    for copy in copies:
        copy.start()

    def send(n, t, source, stride, start):
        def narrow(c, carry):
            tail[n, c] = source[pl.ds(c * stride + start, TILE), :].astype(bf16)
            return carry

        lax.fori_loop(0, channels, narrow, 0, unroll=16)
        copies.append(pltpu.make_async_copy(
            tail.at[n], slope_hbm.at[:, pl.ds(t * TILE, TILE), :], sem.at[3 + n]))
        copies[-1].start()

    beside = tile + 1 - tile % 2 * 2
    send(0, beside, big, pitch, beside * TILE)
    for n in range(TILE // 2):
        y = slope_of(tile * TILE // 2 + n, gs, wb)
        for i in range(2):
            last_rows[pl.ds(2 * n + i, channels, stride=short), :] = y[:, i * cols : (i + 1) * cols]
    send(1, tile, last_rows, short, 0)
    for copy in copies:
        copy.wait()


def shards(layer_inputs, conv_weight, channel_offset, observed, var_weight):
    _, channels, rows, cols = layer_inputs.shape
    outputs = conv_weight.shape[2]
    members, lats, lons = [lax.axis_size(n) for n in ("member", "lat", "lon")]
    tall, padded = -(-outputs // 8) * 8, -(-outputs // 16) * 16
    count, sizes_sent = len(plan(rows)[0]), spans(rows, outputs)[1]
    flat = pltpu.VMEM((tall, cols), f32)
    pitch = pitch_of(rows)
    sizes = (members, lats, lons, channels, rows, cols, outputs, tall, padded)
    vmem = pl.BlockSpec(memory_space=pltpu.VMEM)
    hbm = pl.BlockSpec(memory_space=pl.ANY)
    dma = pltpu.SemaphoreType.DMA
    wide = -(-9 * padded // 128) * 128
    held = (outputs + channels) * rows * cols * 2 + channels * pitch * cols * 4 + 65536
    held += (rows + 2) * 3 * padded * cols * 2 + channels * wide * 2
    predicted, slope, *parts = pl.pallas_call(
        functools.partial(kernel, sizes),
        out_shape=(
            pltpu.VMEM((outputs, rows, cols), bf16),
            pltpu.VMEM((channels, rows, cols), bf16),
            pltpu.VMEM((channels * pitch, cols), f32),
            pltpu.VMEM((rows + 2, 3 * padded, cols), bf16),
            pltpu.VMEM((channels, wide), bf16),
        ),
        in_specs=[hbm] * 5,
        out_specs=(vmem,) * 5,
        scratch_shapes=[
            pltpu.SMEM(channel_offset.shape, f32),
            pltpu.SMEM(var_weight.shape, f32),
            pltpu.VMEM((channels, rows, cols), bf16),
            pltpu.VMEM(conv_weight.shape, bf16),
            pltpu.VMEM((outputs, rows, cols), bf16),
            dma((rows // TILE + 4,)),
            pltpu.VMEM((rows + 2, channels, cols), bf16),
            pltpu.VMEM((3 * padded, 3 * channels), bf16),
            pltpu.VMEM((wide, channels), bf16),
            pltpu.VMEM((tall * pitch, cols), f32),
            pltpu.VMEM((sum(sizes_sent), cols), bf16),
            pltpu.VMEM((max(sizes_sent) + 8, cols), f32),
            pltpu.VMEM((members - 1, sum(sizes_sent), cols), bf16),
            pltpu.VMEM((members - 1, max(sizes_sent) + 8, cols), f32),
            pltpu.VMEM((tall * pitch, cols), f32),
            pltpu.VMEM((rows, tall, cols), f32),
            pltpu.VMEM((rows + 8, cols), f32),
            flat, flat, pltpu.VMEM((2, tall, cols), f32), flat, flat, pltpu.VMEM((tall, cols), bf16),
            pltpu.VMEM((2, tall, cols), bf16),
            pltpu.VMEM((2, 2, tall, cols), bf16),
            pltpu.VMEM((tall, cols), bf16),
            pltpu.VMEM((members - 1, tall, cols), bf16),
            pltpu.VMEM((tall, cols), bf16),
            pltpu.VMEM((2, tall, cols), bf16),
            dma((2,)), dma((2,)), dma((2,)), dma((2,)),
            dma((2, 2)), dma((2, 2)), dma((members - 1,)), dma((members - 1,)), dma((2,)), dma((2,)),
            dma((count, members - 1)), dma((count, members - 1)),
        ],
        compiler_params=pltpu.CompilerParams(
            collective_id=0, has_side_effects=True, vmem_limit_bytes=ROOM - held),
        name="crps_step",
    )(layer_inputs[0], conv_weight, observed, channel_offset, var_weight)
    predicted, slope = pl.pallas_call(
        store,
        out_shape=(
            jax.ShapeDtypeStruct(predicted.shape, bf16),
            jax.ShapeDtypeStruct(slope.shape, bf16),
        ),
        in_specs=[vmem] * 5,
        out_specs=(hbm, hbm),
        scratch_shapes=[
            pltpu.VMEM((channels * pitch_of(TILE), cols), f32),
            pltpu.VMEM((2, channels, TILE, cols), bf16),
            dma((5,)),
        ],
        compiler_params=pltpu.CompilerParams(vmem_limit_bytes=8 * 1024 * 1024),
        name="store",
    )(predicted, slope, *parts)
    return predicted[None], slope[None]


def solution(mesh):
    in_specs = (P("member", None, "lat", "lon"), P(), P(), P(None, "lat", "lon"), P())
    out_specs = (P("member", None, "lat", "lon"), P("member", None, "lat", "lon"))
    return jax.shard_map(shards, mesh=mesh, in_specs=in_specs, out_specs=out_specs, check_vma=False)
```

```python
import functools

import jax
import jax.numpy as jnp
from jax import lax
from jax.experimental import pallas as pl
from jax.experimental.pallas import tpu as pltpu
from jax.sharding import PartitionSpec as P

MESH = pl.DeviceIdType.MESH
smoothing = 0.25
CHUNK = 16
TILE = 8
ROOM = 67_043_328
f32, bf16 = jnp.float32, jnp.bfloat16


def smooth(difference):
    return difference * lax.rsqrt(difference * difference + smoothing * smoothing)


def pitch_of(rows):
    return rows + 1 - rows % 2


def plan(rows):
    pairs, half = rows // 2, CHUNK // 2
    chunks = rows // CHUNK
    if chunks < 3:
        return [list(range(1, pairs - 1)), sorted({0, pairs - 1})], 1
    base = chunks // 2 * half
    core = list(range(base + 1, base + half - 1))
    low, high = list(range(1, base + 1)), list(range(base + half - 1, pairs - 1))
    cut = lambda run: [run[max(i - 4, 0) : i] for i in range(len(run), 0, -4)]
    early = [core[:1], core[1:2], core[2:4], low[-4:], low[-8:-4]]
    late = [[0, pairs - 1]] + cut(low[:-8]) + cut(high) + [[pair] for pair in core[4:]]
    return [g for g in early if g] + [g for g in late if g], len([g for g in early if g])


def spans(rows, outputs):
    sizes = [-(-2 * len(group) * outputs // 8) * 8 for group in plan(rows)[0]]
    return [sum(sizes[:k]) for k in range(len(sizes))], sizes


def final_tile(rows):
    return plan(rows)[0][-1][-1] * 2 // TILE


def slope_of(pair, gs, wb):
    _, depth, cols = gs.shape
    rhs = jnp.concatenate(
        [gs[2 * pair + i : 2 * pair + i + 3].reshape(3 * depth, cols) for i in range(2)], axis=1)
    return jnp.dot(wb[:, : 3 * depth], rhs, preferred_element_type=f32)


def kernel(
    sizes,
    x_hbm, w_hbm, obs_hbm, bias_hbm, var_hbm,
    p_ref, out_ref, big, gs, wb,
    bias_ref, var_ref, x_ref, w_ref, obs_ref, load_sem, xt, wf, wbt, po, pr, stage, others, spare,
    ob, misfits, latw, biasb, varb, partial, border, border_obs, around,
    edge_out, edge_in, rim_out, rim_in, gedge_out, gedge_in,
    row_send, row_recv, grow_send, grow_recv,
    edge_send, edge_recv, rim_send, rim_recv, gedge_send, gedge_recv, peer_send, peer_recv,
):
    members, lats, lons, channels, rows, cols, outputs, tall, padded = sizes
    pitch = pitch_of(rows)
    chunks = rows // CHUNK
    pairs = rows // 2
    groups, ahead_of_rim = plan(rows)
    first, length = spans(rows, outputs)
    last = len(groups) - 1
    outer = [k for k, group in enumerate(groups) if 0 in group or pairs - 1 in group]
    inner = [k for k in range(last + 1) if k not in outer]
    tiles = rows // TILE
    start = groups[0][0] * 2 // TILE if chunks > 2 else 0
    order = [start, 0, tiles - 1] + [t + start for t in range(1, tiles - start)]
    order = list(dict.fromkeys(order + list(range(start, -1, -1))))
    me, lat, lon = lax.axis_index("member"), lax.axis_index("lat"), lax.axis_index("lon")
    right, left = lax.rem(lon + 1, lons), lax.rem(lon + lons - 1, lons)
    has_up, has_down = lat > 0, lat < lats - 1

    barrier = pltpu.get_barrier_semaphore()

    def greet(step, carry):
        other = lax.rem(me + step, members)
        pl.semaphore_signal(barrier, inc=1, device_id=(other, lat, lon), device_id_type=MESH)
        return carry

    lax.fori_loop(1, members, greet, 0)
    for side in (left, right):
        pl.semaphore_signal(barrier, inc=1, device_id=(me, lat, side), device_id_type=MESH)

    @pl.when(has_up)
    def _():
        pl.semaphore_signal(barrier, inc=1, device_id=(me, lat - 1, lon), device_id_type=MESH)

    @pl.when(has_down)
    def _():
        pl.semaphore_signal(barrier, inc=1, device_id=(me, lat + 1, lon), device_id_type=MESH)

    loads = {"bias": pltpu.make_async_copy(bias_hbm, bias_ref, load_sem.at[tiles + 2])}
    for q in order:
        loads[q] = pltpu.make_async_copy(
            x_hbm.at[:, pl.ds(q * TILE, TILE), :], x_ref.at[:, pl.ds(q * TILE, TILE), :],
            load_sem.at[q])
        if q == start:
            loads["w"] = pltpu.make_async_copy(w_hbm, w_ref, load_sem.at[tiles])
    loads["var"] = pltpu.make_async_copy(var_hbm, var_ref, load_sem.at[tiles + 3])
    loads["obs"] = pltpu.make_async_copy(obs_hbm, obs_ref, load_sem.at[tiles + 1])
    for load in loads.values():
        load.start()

    lane = lax.broadcasted_iota(jnp.int32, (tall, cols), 1)
    at_first, at_last = lane == 0, lane == cols - 1
    at_ends = at_first | at_last
    odd = lane % 2 == 1

    def spread(array, source):
        array[...] = jnp.zeros(array.shape, f32)

        def one(o, carry):
            array[pl.ds(o, 1), :] = jnp.full((1, cols), source[o], f32)
            return carry

        lax.fori_loop(0, outputs, one, 0, unroll=3)

    wf[...] = jnp.zeros(wf.shape, bf16)
    border[...] = jnp.zeros(border.shape, f32)
    loads["bias"].wait()
    spread(biasb, bias_ref)

    def unroll_of(n):
        return max(d for d in range(1, 25) if n % d == 0)

    def turn(r, carry):
        xt[r + 1] = big[pl.ds(r, channels, stride=pitch), :].astype(bf16)
        return carry

    def bring(t, low=0, high=TILE):
        loads[t].wait()

        def one(c, carry):
            big[pl.ds(c * pitch + t * TILE, TILE), :] = (
                x_ref[c, t * TILE : (t + 1) * TILE, :].astype(f32))
            return carry

        lax.fori_loop(0, channels, one, 0, unroll=16)
        lax.fori_loop(t * TILE + low, t * TILE + high, turn, 0, unroll=4)

    def row_copies(array, send, recv):
        up = pltpu.make_async_remote_copy(
            src_ref=array.at[1], dst_ref=array.at[rows + 1], send_sem=send.at[0],
            recv_sem=recv.at[0], device_id=(me, lat - 1, lon), device_id_type=MESH)
        down = pltpu.make_async_remote_copy(
            src_ref=array.at[rows], dst_ref=array.at[0], send_sem=send.at[1],
            recv_sem=recv.at[1], device_id=(me, lat + 1, lon), device_id_type=MESH)
        return up, down

    def start_up(copies):
        pl.when(has_up)(lambda: copies[0].start())

    def start_down(copies):
        pl.when(has_down)(lambda: copies[1].start())

    def wait_rows(copies, array):
        @pl.when(has_up)
        def _():
            copies[1].wait_recv()
            copies[0].wait_send()

        @pl.when(has_down)
        def _():
            copies[0].wait_recv()
            copies[1].wait_send()

        @pl.when(lat == 0)
        def _():
            array[0] = jnp.zeros(array.shape[1:], bf16)

        @pl.when(lat == lats - 1)
        def _():
            array[rows + 1] = jnp.zeros(array.shape[1:], bf16)

    def edge_copies(source, target, send, recv):
        return [
            pltpu.make_async_remote_copy(
                src_ref=source, dst_ref=target.at[s], send_sem=send.at[s],
                recv_sem=recv.at[s], device_id=(me, lat, side), device_id_type=MESH)
            for s, side in enumerate((right, left))]

    def to_peers(act):
        def one(step, carry):
            act(step)
            return carry

        lax.fori_loop(1, members, one, 0)

    peer = lambda k, step: pltpu.make_async_remote_copy(
        src_ref=pr.at[pl.ds(first[k], length[k])],
        dst_ref=others.at[step - 1, pl.ds(first[k], length[k])],
        send_sem=peer_send.at[k, step - 1], recv_sem=peer_recv.at[k, step - 1],
        device_id=(lax.rem(me + step, members), lat, lon), device_id_type=MESH)
    rim = lambda step: pltpu.make_async_remote_copy(
        src_ref=rim_out, dst_ref=rim_in.at[step - 1],
        send_sem=rim_send.at[step - 1], recv_sem=rim_recv.at[step - 1],
        device_id=(lax.rem(me + step, members), lat, lon), device_id_type=MESH)
    edges = [
        edge_copies(edge_out.at[n], edge_in.at[n], edge_send.at[n], edge_recv.at[n])
        for n in range(2)]
    gedges = edge_copies(gedge_out, gedge_in, gedge_send, gedge_recv)

    def rows_of(k):
        return [(pair, i, 2 * pair + i) for pair in groups[k] for i in range(2)]

    def forward(k):
        share = jnp.zeros((tall, cols), f32)
        own = jnp.zeros((tall, cols), f32)
        for j, pair in enumerate(groups[k]):
            rhs = jnp.concatenate(
                [xt[2 * pair + i : 2 * pair + i + 3].reshape(3 * channels, cols) for i in range(2)],
                axis=1)
            y = jnp.dot(wf[...], rhs, preferred_element_type=f32)
            for i in range(2):
                r = 2 * pair + i
                from_left, mid, from_right = [
                    y[b * padded : b * padded + tall, i * cols : (i + 1) * cols] for b in range(3)]
                from_left = pltpu.roll(from_left, 1, 1)
                from_right = pltpu.roll(from_right, cols - 1, 1)
                total = mid + biasb[...] + jnp.where(at_first, 0.0, from_left)
                total = total + jnp.where(at_last, 0.0, from_right)
                po[pl.ds(r, tall, stride=pitch), :] = total
                at = (2 * j + i) * outputs
                stage[at : at + tall, :] = total
                both = pltpu.roll(jnp.where(at_first, from_left, from_right), 2 * r + 1, 1)
                mine = lane // 2 == r
                share = jnp.where(mine, both, share)
                own = jnp.where(mine, pltpu.roll(total, 2 * r + 1, 1), own)
        pr[first[k] : first[k] + length[k], :] = stage[0 : length[k], :].astype(bf16)
        at = 1 if k in outer else 0
        partial[at] = share if k in (outer[0], inner[0]) else partial[at] + share
        border[...] = border[...] + own

    def exchange(n):
        edge_out[n] = partial[n].astype(bf16)
        for copy in edges[n]:
            copy.start()

    def enter():
        pl.semaphore_wait(barrier, members + 1 + has_up.astype(jnp.int32) + has_down.astype(jnp.int32))

    x_rows = row_copies(xt, row_send, row_recv)
    waiting = list(order)
    low, high = 0, TILE
    if chunks > 2:
        low, high = groups[0][0] * 2 - 1 - start * TILE, groups[0][-1] * 2 + 3 - start * TILE
    bring(waiting.pop(0), low, high)
    loads["w"].wait()
    for a in range(3):
        for b in range(3):
            wf[b * padded : b * padded + outputs, a * channels : (a + 1) * channels] = w_ref[a, b]
    for n, k in enumerate(inner):
        needed = {r // TILE for pair in groups[k] for r in range(2 * pair - 1, 2 * pair + 3)}
        while needed & set(waiting):
            bring(waiting.pop(0))
        forward(k)
        if n == 0:
            enter()
        if k < ahead_of_rim:
            to_peers(lambda step: peer(k, step).start())
        if n == 0:
            lax.fori_loop(start * TILE, start * TILE + low, turn, 0)
            lax.fori_loop(start * TILE + high, (start + 1) * TILE, turn, 0, unroll=3)
        if n == min(1, len(inner) - 1):
            while {0, tiles - 1} & set(waiting):
                bring(waiting.pop(0))
            start_up(x_rows)
            start_down(x_rows)
    exchange(0)

    border_obs[...] = jnp.zeros(border_obs.shape, f32)
    loads["var"].wait()
    spread(varb, var_ref)

    def blank(r, carry):
        for b in range(3):
            gs[r, b * padded + tall : (b + 1) * padded, :] = jnp.zeros((padded - tall, cols), bf16)
        return carry

    lax.fori_loop(1, rows + 1, blank, 0)
    loads["obs"].wait()

    def widen_obs(o, carry):
        ob[pl.ds(o * pitch, rows), :] = obs_ref[o].astype(f32)
        return carry

    lax.fori_loop(0, outputs, widen_obs, 0, unroll=unroll_of(outputs))
    ob[pl.ds(outputs * pitch, (tall - outputs) * pitch), :] = jnp.zeros(
        ((tall - outputs) * pitch, cols), f32)
    wait_rows(x_rows, xt)
    for k in outer:
        forward(k)
    exchange(1)

    wbt[...] = jnp.zeros(wbt.shape, bf16)
    for a in range(3):
        for b in range(3):
            base = ((2 - a) * 3 + b) * padded
            wbt[base : base + outputs, :] = w_ref[a, b]
    wb[...] = jnp.transpose(wbt[...])

    def latitude(row):
        row_index = (lat * rows + row).astype(f32)
        return jnp.cos((-80.0 + 160.0 * (row_index + 0.5) / float(rows * lats)) * (jnp.pi / 180.0))

    latw[0:rows, :] = latitude(lax.broadcasted_iota(jnp.int32, (rows, cols), 0))
    latw[rows : rows + 8, :] = latitude(lax.broadcasted_iota(jnp.int32, (8, cols), 1) // 2)

    def gather_obs(k):
        own = jnp.zeros((tall, cols), f32)
        for _, _, r in rows_of(k):
            turned = pltpu.roll(ob[pl.ds(r, tall, stride=pitch), :], 2 * r + 1, 1)
            own = jnp.where(lane // 2 == r, turned, own)
        border_obs[...] = border_obs[...] + own

    for k in range(last + 1):
        gather_obs(k)

    arrived = jnp.zeros((tall, cols), f32)
    for n in range(2):
        for copy in edges[n]:
            copy.wait()
        arrived = arrived + jnp.where(odd, edge_in[n, 0].astype(f32), edge_in[n, 1].astype(f32))
    rim_out[...] = (border[...] + arrived).astype(bf16)
    to_peers(lambda step: rim(step).start())
    for k in range(last + 1):
        if k >= ahead_of_rim or k in outer:
            to_peers(lambda step: peer(k, step).start())

    def complete(k):
        rim_own = rim_out[...].astype(f32)
        for pair, i, r in rows_of(k):
            own = po[pl.ds(r, tall, stride=pitch), :]
            own = jnp.where(at_ends, pltpu.roll(rim_own, cols - 1 - 2 * r, 1), own)
            own = own.astype(bf16).astype(f32)
            misfits[r] = smooth(own - ob[pl.ds(r, tall, stride=pitch), :])
            po[pl.ds(r, tall, stride=pitch), :] = own

    for k in range(last + 1):
        complete(k)

    def pack(o, carry):
        p_ref[o] = po[pl.ds(o * pitch, rows), :].astype(bf16)
        return carry

    lax.fori_loop(0, outputs, pack, 0, unroll=unroll_of(outputs))

    def spread_sum(own, other):
        add = lambda n, run: run + smooth(own - other(n))
        pair_sum = smooth(own - own)
        if members == 2:
            pair_sum = add(0, pair_sum)
        else:
            pair_sum = lax.fori_loop(0, members - 1, add, pair_sum)
        return pair_sum / (members - 1)

    to_peers(lambda step: rim(step).wait())
    rim_own = rim_out[...].astype(f32)
    value = smooth(rim_own - border_obs[...]) - spread_sum(rim_own, lambda n: rim_in[n].astype(f32))
    value = latw[rows : rows + 1, :] * varb[...] * value
    value = jnp.where(odd, pltpu.roll(value, 1, 1), pltpu.roll(value, cols - 1, 1))
    gedge_out[...] = value.astype(bf16)
    for copy in gedges:
        copy.start()
    for copy in gedges:
        copy.wait()
    around[...] = jnp.where(odd, gedge_in[0], gedge_in[1])

    g_rows = row_copies(gs, grow_send, grow_recv)
    ready, done, packed = set(), set(), set()
    left_over = [final_tile(rows) * TILE // 2 + n for n in range(TILE // 2)]

    def gradient(k):
        to_peers(lambda step: peer(k, step).wait())

        def unfold(n, carry):
            spare[n, 0 : length[k], :] = others[n, first[k] : first[k] + length[k], :].astype(f32)
            spare[n, length[k] : length[k] + 8, :] = jnp.zeros((8, cols), f32)
            return carry

        lax.fori_loop(0, members - 1, unfold, 0)
        for j, (_, _, r) in enumerate(rows_of(k)):

            def other(n):
                patch = pltpu.roll(rim_in[n], cols - 1 - 2 * r, 1)
                theirs = spare[n, j * outputs : j * outputs + tall, :]
                return jnp.where(at_ends, patch.astype(f32), theirs)

            own = po[pl.ds(r, tall, stride=pitch), :]
            value = latw[r : r + 1, :] * varb[...] * (misfits[r] - spread_sum(own, other))
            value = value.astype(bf16)
            both = pltpu.roll(around[...], cols - 1 - 2 * r, 1)
            gs[r + 1, 0:tall, :] = jnp.where(at_last, both, pltpu.roll(value, cols - 1, 1))
            gs[r + 1, padded : padded + tall, :] = value
            gs[r + 1, 2 * padded : 2 * padded + tall, :] = jnp.where(
                at_first, both, pltpu.roll(value, 1, 1))
            ready.add(r)
        if 0 in groups[k]:
            start_up(g_rows)
        if pairs - 1 in groups[k]:
            start_down(g_rows)

    def backward():
        for pair in range(pairs):
            if pair in left_over or pair in done or not {2 * pair - 1, 2 * pair, 2 * pair + 1, 2 * pair + 2} <= ready:
                continue
            done.add(pair)
            y = slope_of(pair, gs, wb)
            for i in range(2):
                big[pl.ds(2 * pair + i, channels, stride=pitch), :] = y[:, i * cols : (i + 1) * cols]
        for q in range(chunks):
            if q == final_tile(rows) * TILE // CHUNK or q in packed or not set(range(q * CHUNK // 2, (q + 1) * CHUNK // 2)) <= done:
                continue
            packed.add(q)

            def narrow(c, carry):
                out_ref[c, q * CHUNK : (q + 1) * CHUNK, :] = (
                    big[pl.ds(c * pitch + q * CHUNK, CHUNK), :].astype(bf16))
                return carry

            lax.fori_loop(0, channels, narrow, 0, unroll=16)

    sequence = outer + inner
    for k in sequence:
        if k == sequence[-2] and k not in outer:
            wait_rows(g_rows, gs)
            ready.update((-1, rows))
            backward()
        gradient(k)
        backward()
    if -1 not in ready:
        wait_rows(g_rows, gs)
        ready.update((-1, rows))
        backward()


def store(p_ref, slope_ref, big, gs, wb, p_hbm, slope_hbm, last_rows, tail, sem):
    channels, rows, cols = slope_ref.shape
    pitch, short = pitch_of(rows), pitch_of(TILE)
    tile = final_tile(rows)
    chunk = tile * TILE // CHUNK * CHUNK
    above, below = pl.ds(0, chunk), pl.ds(chunk + CHUNK, rows - chunk - CHUNK)
    copies = [pltpu.make_async_copy(p_ref, p_hbm, sem.at[0])]
    for n, part in enumerate((above, below)):
        if part.size:
            copies.append(pltpu.make_async_copy(
                slope_ref.at[:, part, :], slope_hbm.at[:, part, :], sem.at[1 + n]))
    for copy in copies:
        copy.start()

    def send(n, t, source, stride, start):
        def narrow(c, carry):
            tail[n, c] = source[pl.ds(c * stride + start, TILE), :].astype(bf16)
            return carry

        lax.fori_loop(0, channels, narrow, 0, unroll=16)
        copies.append(pltpu.make_async_copy(
            tail.at[n], slope_hbm.at[:, pl.ds(t * TILE, TILE), :], sem.at[3 + n]))
        copies[-1].start()

    beside = tile + 1 - tile % 2 * 2
    send(0, beside, big, pitch, beside * TILE)
    for n in range(TILE // 2):
        y = slope_of(tile * TILE // 2 + n, gs, wb)
        for i in range(2):
            last_rows[pl.ds(2 * n + i, channels, stride=short), :] = y[:, i * cols : (i + 1) * cols]
    send(1, tile, last_rows, short, 0)
    for copy in copies:
        copy.wait()


def shards(layer_inputs, conv_weight, channel_offset, observed, var_weight):
    _, channels, rows, cols = layer_inputs.shape
    outputs = conv_weight.shape[2]
    members, lats, lons = [lax.axis_size(n) for n in ("member", "lat", "lon")]
    tall, padded = -(-outputs // 8) * 8, -(-outputs // 16) * 16
    count, sizes_sent = len(plan(rows)[0]), spans(rows, outputs)[1]
    flat = pltpu.VMEM((tall, cols), f32)
    pitch = pitch_of(rows)
    sizes = (members, lats, lons, channels, rows, cols, outputs, tall, padded)
    vmem = pl.BlockSpec(memory_space=pltpu.VMEM)
    hbm = pl.BlockSpec(memory_space=pl.ANY)
    dma = pltpu.SemaphoreType.DMA
    wide = -(-9 * padded // 128) * 128
    held = (outputs + channels) * rows * cols * 2 + channels * pitch * cols * 4 + 65536
    held += (rows + 2) * 3 * padded * cols * 2 + channels * wide * 2
    predicted, slope, *parts = pl.pallas_call(
        functools.partial(kernel, sizes),
        out_shape=(
            pltpu.VMEM((outputs, rows, cols), bf16),
            pltpu.VMEM((channels, rows, cols), bf16),
            pltpu.VMEM((channels * pitch, cols), f32),
            pltpu.VMEM((rows + 2, 3 * padded, cols), bf16),
            pltpu.VMEM((channels, wide), bf16),
        ),
        in_specs=[hbm] * 5,
        out_specs=(vmem,) * 5,
        scratch_shapes=[
            pltpu.SMEM(channel_offset.shape, f32),
            pltpu.SMEM(var_weight.shape, f32),
            pltpu.VMEM((channels, rows, cols), bf16),
            pltpu.VMEM(conv_weight.shape, bf16),
            pltpu.VMEM((outputs, rows, cols), bf16),
            dma((rows // TILE + 4,)),
            pltpu.VMEM((rows + 2, channels, cols), bf16),
            pltpu.VMEM((3 * padded, 3 * channels), bf16),
            pltpu.VMEM((wide, channels), bf16),
            pltpu.VMEM((tall * pitch, cols), f32),
            pltpu.VMEM((sum(sizes_sent), cols), bf16),
            pltpu.VMEM((max(sizes_sent) + 8, cols), f32),
            pltpu.VMEM((members - 1, sum(sizes_sent), cols), bf16),
            pltpu.VMEM((members - 1, max(sizes_sent) + 8, cols), f32),
            pltpu.VMEM((tall * pitch, cols), f32),
            pltpu.VMEM((rows, tall, cols), f32),
            pltpu.VMEM((rows + 8, cols), f32),
            flat, flat, pltpu.VMEM((2, tall, cols), f32), flat, flat, pltpu.VMEM((tall, cols), bf16),
            pltpu.VMEM((2, tall, cols), bf16),
            pltpu.VMEM((2, 2, tall, cols), bf16),
            pltpu.VMEM((tall, cols), bf16),
            pltpu.VMEM((members - 1, tall, cols), bf16),
            pltpu.VMEM((tall, cols), bf16),
            pltpu.VMEM((2, tall, cols), bf16),
            dma((2,)), dma((2,)), dma((2,)), dma((2,)),
            dma((2, 2)), dma((2, 2)), dma((members - 1,)), dma((members - 1,)), dma((2,)), dma((2,)),
            dma((count, members - 1)), dma((count, members - 1)),
        ],
        compiler_params=pltpu.CompilerParams(
            collective_id=0, has_side_effects=True, vmem_limit_bytes=ROOM - held),
        name="crps_step",
    )(layer_inputs[0], conv_weight, observed, channel_offset, var_weight)
    predicted, slope = pl.pallas_call(
        store,
        out_shape=(
            jax.ShapeDtypeStruct(predicted.shape, bf16),
            jax.ShapeDtypeStruct(slope.shape, bf16),
        ),
        in_specs=[vmem] * 5,
        out_specs=(hbm, hbm),
        scratch_shapes=[
            pltpu.VMEM((channels * pitch_of(TILE), cols), f32),
            pltpu.VMEM((2, channels, TILE, cols), bf16),
            dma((5,)),
        ],
        compiler_params=pltpu.CompilerParams(vmem_limit_bytes=8 * 1024 * 1024),
        name="store",
    )(predicted, slope, *parts)
    return predicted[None], slope[None]


def solution(mesh):
    in_specs = (P("member", None, "lat", "lon"), P(), P(), P(None, "lat", "lon"), P())
    out_specs = (P("member", None, "lat", "lon"), P("member", None, "lat", "lon"))
    return jax.shard_map(shards, mesh=mesh, in_specs=in_specs, out_specs=out_specs, check_vma=False)
```
